128 devices in a mesh: row: 8 (over x, core), col: 16 (over z, y).
Axes of the slice: x: 4, y: 4, z: 4, core: 2. Of those that a mesh axis runs over, the one named last changes fastest.
Arguments:
- concentration: float32 [256, 256, 256], P('row', 'col'), may hold values from 0 to 1
Outputs:
- concentration_next: float32 [256, 256, 256], P('row', 'col')
- strain: float32 [6, 256, 256, 256], P(None, 'row', 'col')
- residual_norms: float32 [2], replicated
The draws below stay inside these ranges and needn't reach their ends.
All inputs are finite; a program needn't handle non-finite values.
Results may differ from the reference program's by a relative error of at most 0.0003.
Values sent between devices are 32-bit elements; how exact they have to be, the bound alone decides.
A program may use at most 192 MiB of HBM per device.

```python
import math
import jax
import jax.numpy as jnp

GRID = 256
ITERS = 2


def draw_concentration(key, part):
    noise_key = jax.random.fold_in(key, 11)
    index = jnp.arange(GRID, dtype=jnp.int32).astype(jnp.float32)
    ramp = 0.1 + 0.2 * (index[:, None, None] + index[None, :, None]) / (2.0 * (GRID - 1))
    rough = jax.random.uniform(noise_key, (GRID, GRID, GRID), jnp.float32, -1.0, 1.0)
    return 0.5 + ramp * rough


def setup_inputs(seed: int = 0) -> dict:
    streams_of = jax.random.split(jax.random.key(seed), 2)
    return {
        "concentration": draw_concentration(jax.random.fold_in(streams_of[1], 71), 0),
    }


FIRST_LOW = 1.0
FIRST_RISE = 0.6
SHEAR_LOW = 0.7
SHEAR_RISE = 0.8
FIRST_REF = 1.3
SHEAR_REF = 1.1
BETA_REF = 2.4 / 3.5
EIGEN_STRAIN = 0.5
WELL_HEIGHT = 1.0
TIME_STEP = 0.5
GRADIENT_ENERGY = 0.5

def moduli(conc):
    return (FIRST_LOW + FIRST_RISE * conc, SHEAR_LOW + SHEAR_RISE * conc)

def polarization(strain, conc):
    first, shear = moduli(conc)
    trace = strain[0] + strain[1] + strain[2]
    normal = (first - FIRST_REF) * trace - (3.0 * first + 2.0 * shear) * EIGEN_STRAIN * conc
    excess = 2.0 * (shear - SHEAR_REF)
    return jnp.stack([normal + excess * strain[0], normal + excess * strain[1], normal + excess * strain[2], excess * strain[3], excess * strain[4], excess * strain[5]])

def green_operator(tau, wave_x, wave_y, wave_z):
    square = wave_x * wave_x + wave_y * wave_y + wave_z * wave_z
    nonzero = square > 0.0
    safe = jnp.where(nonzero, square, 1.0)
    scale = jnp.where(nonzero, 1.0 / (SHEAR_REF * safe), 0.0)
    force_x = tau[0] * wave_x + tau[5] * wave_y + tau[4] * wave_z
    force_y = tau[5] * wave_x + tau[1] * wave_y + tau[3] * wave_z
    force_z = tau[4] * wave_x + tau[3] * wave_y + tau[2] * wave_z
    along = (wave_x * force_x + wave_y * force_y + wave_z * force_z) * (BETA_REF / safe)
    moved_x = scale * (force_x - along * wave_x)
    moved_y = scale * (force_y - along * wave_y)
    moved_z = scale * (force_z - along * wave_z)
    return jnp.stack([-wave_x * moved_x, -wave_y * moved_y, -wave_z * moved_z, -0.5 * (wave_y * moved_z + wave_z * moved_y), -0.5 * (wave_x * moved_z + wave_z * moved_x), -0.5 * (wave_x * moved_y + wave_y * moved_x)])

def potential(strain, conc):
    first, shear = moduli(conc)
    dilation = EIGEN_STRAIN * conc
    part_x = strain[0] - dilation
    part_y = strain[1] - dilation
    part_z = strain[2] - dilation
    trace = part_x + part_y + part_z
    energy = part_x * part_x + part_y * part_y + part_z * part_z + 2.0 * (strain[3] * strain[3] + strain[4] * strain[4] + strain[5] * strain[5])
    chemical = 2.0 * WELL_HEIGHT * conc * (1.0 - conc) * (1.0 - 2.0 * conc)
    return chemical + 0.5 * FIRST_RISE * trace * trace + SHEAR_RISE * energy - EIGEN_STRAIN * (3.0 * first + 2.0 * shear) * trace

def forward_full(fields, half_length):
    return jnp.fft.rfftn(fields, axes=(-3, -2, -1))[..., :half_length]

def inverse_full(spectrum, length):
    padded = jnp.concatenate([spectrum, jnp.zeros(spectrum.shape[:-1] + (1,), spectrum.dtype)], axis=-1)
    return jnp.fft.irfftn(padded, s=(length, length, length), axes=(-3, -2, -1))

def reference(concentration):
    half_length = GRID // 2
    index = jnp.arange(GRID, dtype=jnp.int32)
    signed = jnp.where(index < half_length, index, index - GRID).astype(jnp.float32) * (2.0 * math.pi / GRID)
    wave_x = signed[:, None, None]
    wave_y = signed[None, :, None]
    wave_z = (jnp.arange(half_length, dtype=jnp.int32).astype(jnp.float32) * (2.0 * math.pi / GRID))[None, None, :]
    strain = jnp.zeros((6, GRID, GRID, GRID), jnp.float32)
    norms = []
    for sweep in range(ITERS):
        tau = polarization(strain, concentration)
        updated = inverse_full(green_operator(forward_full(tau, half_length), wave_x, wave_y, wave_z), GRID)
        change = updated - strain
        norms.append(jnp.sqrt(jnp.sum(change * change) / GRID ** 3))
        strain = updated
    drive = potential(strain, concentration)
    square = wave_x * wave_x + wave_y * wave_y + wave_z * wave_z
    spectrum = (forward_full(concentration, half_length) - TIME_STEP * square * forward_full(drive, half_length)) / (1.0 + TIME_STEP * GRADIENT_ENERGY * square * square)
    concentration_next = inverse_full(spectrum, GRID)
    return (concentration_next, strain, jnp.stack(norms))
```

```python
import math

import jax
import jax.numpy as jnp
import numpy as np
from jax import lax
from jax.experimental import pallas as pl
from jax.experimental.pallas import tpu as pltpu
from jax.sharding import PartitionSpec as P

F32 = jnp.float32
B16 = jnp.bfloat16
N = 256
H = 128
ITERS = 2
STEP = 2.0 * math.pi / N
SCALE = 1.0 / float(N) ** 3

FIRST_LOW = 1.0
FIRST_RISE = 0.6
SHEAR_LOW = 0.7
SHEAR_RISE = 0.8
FIRST_REF = 1.3
SHEAR_REF = 1.1
BETA_REF = 2.4 / 3.5
EIGEN_STRAIN = 0.5
WELL_HEIGHT = 1.0
TIME_STEP = 0.5
GRADIENT_ENERGY = 0.5

XX, YY, ZZ, YZ, XZ, XY = range(6)


def base_tables():
    index = np.arange(N)
    angle = (index[:, None] * index[None, :] % N) * (2.0 * np.pi / N)
    parts = []
    for table in (np.cos(angle), np.sin(angle)):
        lead = table.astype(np.float32).astype(jnp.bfloat16)
        rest = (table - lead.astype(np.float64)).astype(np.float32).astype(jnp.bfloat16)
        parts += [lead, rest]
    return np.stack(parts)


def split(value):
    lead = value.astype(B16)
    rest = (value - lead.astype(F32)).astype(B16)
    return lead, rest


def dot(a, b):
    return jnp.dot(a, b, preferred_element_type=F32)


def fill_left(base, out, sine_sign):
    for block, part in enumerate((0, 0, 1)):
        at = block * 2 * N
        cosine, sine = base[part], base[2 + part]
        upper, lower = (sine, -sine) if sine_sign > 0 else (-sine, sine)
        out[0:N, at : at + N] = cosine
        out[0:N, at + N : at + 2 * N] = upper
        out[N : 2 * N, at : at + N] = lower
        out[N : 2 * N, at + N : at + 2 * N] = cosine


def fill_right(base, out, sine_sign):
    for block, part in enumerate((0, 0, 1)):
        at = block * 2 * N
        cosine, sine = base[part], base[2 + part]
        upper, lower = (sine, -sine) if sine_sign > 0 else (-sine, sine)
        out[at : at + N, 0:N] = cosine
        out[at : at + N, N : 2 * N] = upper
        out[at + N : at + 2 * N, 0:N] = lower
        out[at + N : at + 2 * N, N : 2 * N] = cosine


def fill_z_ahead(base, out):
    for block, part in enumerate((0, 0, 1)):
        at = block * N
        out[0:H, at : at + N] = base[part, 0:H, :]
        out[H:N, at : at + N] = -base[2 + part, 0:H, :]


def fill_z_back(base, out):
    column = lax.broadcasted_iota(jnp.int32, (N, H), 1)
    weight = jnp.where(column == 0, 1.0, 2.0)
    for block, part in enumerate((0, 0, 1)):
        at = block * N
        out[:, at : at + H] = (base[part, :, 0:H].astype(F32) * weight).astype(B16)
        out[:, at + H : at + N] = (base[2 + part, :, 0:H].astype(F32) * -weight).astype(B16)


def put_pair(wide, x, real, imag):
    rows = pl.ds(x * H, H)
    for at, value in ((0, real), (N, imag)):
        lead, rest = split(value)
        wide[rows, at : at + N] = lead
        wide[rows, 2 * N + at : 3 * N + at] = rest
        wide[rows, 4 * N + at : 5 * N + at] = lead


def z_ahead(field, z_table, tall, wide, x):
    lead, rest = split(field)
    tall[0:N, :] = lead
    tall[N : 2 * N, :] = rest
    tall[2 * N : 3 * N, :] = lead
    spectrum = dot(z_table[...], tall[0 : 3 * N, :])
    put_pair(wide, x, spectrum[0:H], spectrum[H:N])


def z_back(real, imag, z_table, tall):
    for at, value in ((0, real), (H, imag)):
        lead, rest = split(value)
        tall[at : at + H, :] = lead
        tall[N + at : N + at + H, :] = rest
        tall[2 * N + at : 2 * N + at + H, :] = lead
    return dot(z_table[...], tall[0 : 3 * N, :])


def store_planes(out, field, spectrum):
    for x in range(2):
        for block in range(4):
            out[field, pl.ds(x * 4 + block, H, stride=8), :] = spectrum[
                x * H : (x + 1) * H, block * H : (block + 1) * H
            ]


def load_plane(landed, field, x):
    parts = [landed[field, pl.ds(x * 4 + block, H, stride=8), :] for block in range(4)]
    return jnp.concatenate(parts[0:2], axis=1), jnp.concatenate(parts[2:4], axis=1)


def x_ahead(landed, field, x_table, tall, spectrum, slot):
    for part in range(2):
        for half in range(2):
            rows = landed[field, pl.ds(part * 2 + half, N, stride=4), :]
            lead, rest = split(rows)
            at, lanes = part * N, slice(half * H, (half + 1) * H)
            tall[at : at + N, lanes] = lead
            tall[2 * N + at : 3 * N + at, lanes] = rest
            tall[4 * N + at : 5 * N + at, lanes] = lead
    spectrum[slot] = dot(x_table[...], tall[...])


def x_back(spectrum, slot, x_table, tall, out, field):
    lead, rest = split(spectrum[slot])
    tall[0 : 2 * N, :] = lead
    tall[2 * N : 4 * N, :] = rest
    tall[4 * N : 6 * N, :] = lead
    lines = dot(x_table[...], tall[...])
    for part in range(2):
        for half in range(2):
            out[field, pl.ds(part * 2 + half, N, stride=4), :] = lines[
                part * N : (part + 1) * N, half * H : (half + 1) * H
            ]


def signed(index):
    return jnp.where(index < H, index, index - N).astype(F32) * STEP


def lane_wave(rows, lanes=N):
    return signed(lax.broadcasted_iota(jnp.int32, (rows, lanes), 1))


def row_wave_z():
    return lax.broadcasted_iota(jnp.int32, (H, N), 0).astype(F32) * STEP


CHUNK = 32


def chunk_waves(chunk, kz):
    row = chunk * CHUNK + lax.broadcasted_iota(jnp.int32, (CHUNK, N), 0)
    wave_x = signed(row)
    wave_y = lane_wave(CHUNK)
    wave_z = kz.astype(F32) * STEP
    square = wave_x * wave_x + wave_y * wave_y + wave_z * wave_z
    return wave_x, wave_y, wave_z, square


def green_first(spectrum, source, kz):
    def body(chunk, _):
        wave_x, wave_y, wave_z, square = chunk_waves(chunk, kz)
        nonzero = square > 0.0
        safe = jnp.where(nonzero, square, 1.0)
        factor = jnp.where(nonzero, (BETA_REF - 1.0) * SCALE / (SHEAR_REF * safe), 0.0)
        for part in range(2):
            rows = pl.ds(part * N + chunk * CHUNK, CHUNK)
            psi = spectrum[source, rows, :] * factor
            once = wave_x * psi
            spectrum[0, rows, :] = wave_x * once
            spectrum[1, rows, :] = once
            spectrum[2, rows, :] = psi
        return 0

    lax.fori_loop(0, N // CHUNK, body, 0)


def green_full(spectrum, kz):
    def body(chunk, _):
        wave_x, wave_y, wave_z, square = chunk_waves(chunk, kz)
        nonzero = square > 0.0
        safe = jnp.where(nonzero, square, 1.0)
        scale = jnp.where(nonzero, -SCALE / (SHEAR_REF * safe), 0.0)
        ratio = BETA_REF / safe
        for part in range(2):
            rows = pl.ds(part * N + chunk * CHUNK, CHUNK)
            first, second, third = (spectrum[slot, rows, :] for slot in range(3))
            force_x = wave_x * first + wave_y * second + wave_z * third
            force_y = wave_x * second + spectrum[3, rows, :]
            force_z = wave_x * third + spectrum[4, rows, :]
            along = (wave_x * force_x + wave_y * force_y + wave_z * force_z) * ratio
            moved_x = scale * (force_x - along * wave_x)
            moved_y = scale * (force_y - along * wave_y)
            moved_z = scale * (force_z - along * wave_z)
            spectrum[0, rows, :] = wave_x * moved_x
            spectrum[1, rows, :] = moved_y
            spectrum[2, rows, :] = moved_z
            spectrum[3, rows, :] = 0.5 * (wave_x * moved_z + wave_z * moved_x)
            spectrum[4, rows, :] = 0.5 * (wave_x * moved_y + wave_y * moved_x)
        return 0

    lax.fori_loop(0, N // CHUNK, body, 0)


def relax(spectrum, drive, conc, kz):
    def body(chunk, _):
        _, _, _, square = chunk_waves(chunk, kz)
        inverse = SCALE / (1.0 + TIME_STEP * GRADIENT_ENERGY * square * square)
        for part in range(2):
            rows = pl.ds(part * N + chunk * CHUNK, CHUNK)
            value = conc[rows, :] - TIME_STEP * square * spectrum[drive, rows, :]
            spectrum[drive, rows, :] = value * inverse
        return 0

    lax.fori_loop(0, N // CHUNK, body, 0)


ROWS = 32


def eigen_stress(conc):
    rise = (3.0 * FIRST_RISE + 2.0 * SHEAR_RISE) * EIGEN_STRAIN
    low = (3.0 * FIRST_LOW + 2.0 * SHEAR_LOW) * EIGEN_STRAIN
    return (0.5 - conc) * (rise * (conc + 0.5) + low)


def polarize(parts, conc):
    first = FIRST_LOW + FIRST_RISE * conc
    excess = 2.0 * (SHEAR_LOW + SHEAR_RISE * conc - SHEAR_REF)
    normal = (first - FIRST_REF) * (parts[0] + parts[1] + parts[2]) + eigen_stress(conc)
    return [normal + excess * p for p in parts[:3]] + [excess * p for p in parts[3:]]


def potential(parts, conc):
    first = FIRST_LOW + FIRST_RISE * conc
    shear = SHEAR_LOW + SHEAR_RISE * conc
    dilation = EIGEN_STRAIN * conc
    d = [p - dilation for p in parts[:3]]
    trace = d[0] + d[1] + d[2]
    energy = d[0] * d[0] + d[1] * d[1] + d[2] * d[2]
    energy = energy + 2.0 * (parts[3] * parts[3] + parts[4] * parts[4] + parts[5] * parts[5])
    chemical = 2.0 * WELL_HEIGHT * conc * (1.0 - conc) * (1.0 - 2.0 * conc)
    return (
        chemical
        + 0.5 * FIRST_RISE * trace * trace
        + SHEAR_RISE * energy
        - EIGEN_STRAIN * (3.0 * first + 2.0 * shear) * trace
    )


def ahead_first(plain, conc, eigen):
    for x in range(2):
        conc[x] = plain[x].T

        def body(chunk, _):
            rows = pl.ds(chunk * ROWS, ROWS)
            eigen[x, rows, :] = eigen_stress(conc[x, rows, :])
            return 0

        lax.fori_loop(0, N // ROWS, body, 0)


def field_ahead(field_of, z_table, y_table, tall, wide):
    for x in range(2):
        z_ahead(field_of(x), z_table, tall, wide, x)
    return dot(wide[...], y_table[...])


def field_back(parts_of, factor, y_table, z_table, tall, wide, out):
    for x in range(2):
        put_pair(wide, x, *parts_of(x))
    lines = dot(wide[...], y_table[...])
    for x in range(2):
        real, imag = lines[x * H : (x + 1) * H, 0:N], lines[x * H : (x + 1) * H, N : 2 * N]
        if factor is not None:
            real, imag = factor * real, factor * imag
        out(x, z_back(real, imag, z_table, tall))


def strain_first(landed, y_back, z_back_table, tall, wide, strain):
    wave_y, wave_z = lane_wave(H), row_wave_z()

    def scaled(field, power):
        def parts_of(x):
            real, imag = load_plane(landed, field, x)
            for _ in range(power):
                real, imag = wave_y * real, wave_y * imag
            return real, imag

        return parts_of

    for target, field, power, factor in (
        (XX, 0, 0, None),
        (XY, 1, 1, None),
        (XZ, 1, 0, wave_z),
        (YY, 2, 2, None),
        (YZ, 2, 1, wave_z),
        (ZZ, 2, 0, wave_z * wave_z),
    ):

        def put(x, value, target=target):
            strain[target, x] = value

        field_back(scaled(field, power), factor, y_back, z_back_table, tall, wide, put)


def strain_full(landed, y_back, z_back_table, tall, wide, strain):
    wave_y, wave_z = lane_wave(H), row_wave_z()

    def plain(field):
        return lambda x: load_plane(landed, field, x)

    def along_y(x):
        real, imag = load_plane(landed, 1, x)
        return wave_y * real, wave_y * imag

    def shear(x):
        real_y, imag_y = load_plane(landed, 1, x)
        real_z, imag_z = load_plane(landed, 2, x)
        return (
            0.5 * (wave_y * real_z + wave_z * real_y),
            0.5 * (wave_y * imag_z + wave_z * imag_y),
        )

    for target, parts_of, factor in (
        (XX, plain(0), None),
        (XZ, plain(3), None),
        (XY, plain(4), None),
        (YY, along_y, None),
        (YZ, shear, None),
        (ZZ, plain(2), wave_z),
    ):

        def put(x, value, target=target):
            strain[target, x] = value

        field_back(parts_of, factor, y_back, z_back_table, tall, wide, put)


def sum_squares(parts):
    total = parts[0] * parts[0]
    for part in parts[1:]:
        total = total + part * part
    return total


def k1(base, plain, conc, out, eigen, tall, wide, z_table, y_table):
    fill_z_ahead(base, z_table)
    fill_right(base, y_table, -1)
    ahead_first(plain, conc, eigen)
    store_planes(out, 0, field_ahead(lambda x: eigen[x], z_table, y_table, tall, wide))
    store_planes(out, 1, field_ahead(lambda x: conc[x], z_table, y_table, tall, wide))


def plane_z():
    return lax.axis_index("row") * 16 + lax.axis_index("col")


def k2(base, landed, out, conc, spectrum, tall, ahead, back):
    fill_left(base, ahead, 1)
    fill_left(base, back, -1)
    x_ahead(landed, 0, ahead, tall, spectrum, 3)
    green_first(spectrum, 3, plane_z())
    for slot in range(3):
        x_back(spectrum, slot, back, tall, out, slot)
    x_ahead(landed, 1, ahead, tall, spectrum, 3)
    conc[...] = spectrum[3]


def k3(base, landed, conc, out, strain, partial, work, planes, tall, wide, zf, zb, yf, yb):
    fill_z_ahead(base, zf)
    fill_z_back(base, zb)
    fill_right(base, yf, -1)
    fill_right(base, yb, 1)
    strain_first(landed, yb, zb, tall, wide, strain)
    partial[...] = jnp.zeros_like(partial)
    for x in range(2):

        def body(chunk, _):
            rows = pl.ds(chunk * ROWS, ROWS)
            parts = [strain[i, x, rows, :] for i in range(6)]
            partial[...] += sum_squares(parts)
            for i, value in enumerate(polarize(parts, conc[x, rows, :])):
                work[i, x, rows, :] = value
            return 0

        lax.fori_loop(0, N // ROWS, body, 0)
    stress_ahead(work, out, planes, tall, wide, zf, yf)


def stress_ahead(work, out, planes, tall, wide, zf, yf):
    wave_y = lane_wave(H)
    wave_y = jnp.concatenate([wave_y, wave_y], axis=1)
    wave_y = jnp.concatenate([wave_y, wave_y], axis=0)
    row = lax.broadcasted_iota(jnp.int32, (N, 2 * N), 0)
    wave_z = jnp.where(row < H, row, row - H).astype(F32) * STEP

    def spectrum_of(component):
        return field_ahead(lambda x: work[component, x], zf, yf, tall, wide)

    store_planes(out, 0, spectrum_of(XX))
    store_planes(out, 1, spectrum_of(XY))
    store_planes(out, 2, spectrum_of(XZ))
    planes[...] = spectrum_of(YZ)
    store_planes(out, 3, wave_y * spectrum_of(YY) + wave_z * planes[...])
    store_planes(out, 4, wave_z * spectrum_of(ZZ) + wave_y * planes[...])


def k4(base, landed, out, spectrum, tall, ahead, back):
    fill_left(base, ahead, 1)
    fill_left(base, back, -1)

    def go(slot, _):
        x_ahead(landed, slot, ahead, tall, spectrum, slot)
        return 0

    lax.fori_loop(0, 5, go, 0)
    green_full(spectrum, plane_z())

    def come(slot, _):
        x_back(spectrum, slot, back, tall, out, slot)
        return 0

    lax.fori_loop(0, 5, come, 0)


def k5(base, landed, conc, before, out, strain, partial, work, drive, tall, wide, zf, zb, yf, yb):
    fill_z_ahead(base, zf)
    fill_z_back(base, zb)
    fill_right(base, yf, -1)
    fill_right(base, yb, 1)
    strain_full(landed, yb, zb, tall, wide, work)
    partial[...] = jnp.zeros_like(partial)
    for x in range(2):

        def body(chunk, _):
            rows = pl.ds(chunk * ROWS, ROWS)
            parts = [work[i, x, rows, :] for i in range(6)]
            partial[...] += sum_squares([p - before[i, x, rows, :] for i, p in enumerate(parts)])
            drive[x, rows, :] = potential(parts, conc[x, rows, :])
            return 0

        lax.fori_loop(0, N // ROWS, body, 0)
    store_planes(out, 0, field_ahead(lambda x: drive[x], zf, yf, tall, wide))

    def turn(i, _):
        for x in range(2):
            strain[i, x] = work[i, x].T
        return 0

    lax.fori_loop(0, 6, turn, 0)


def k6(base, landed, conc, out, spectrum, tall, ahead, back):
    fill_left(base, ahead, 1)
    fill_left(base, back, -1)
    x_ahead(landed, 0, ahead, tall, spectrum, 0)
    relax(spectrum, 0, conc, plane_z())
    x_back(spectrum, 0, back, tall, out, 0)


def k7(base, landed, plain, tall, wide, zb, yb):
    fill_z_back(base, zb)
    fill_right(base, yb, 1)

    def put(x, value):
        plain[x] = value.T

    field_back(lambda x: load_plane(landed, 0, x), None, yb, zb, tall, wide, put)


TALL = pltpu.VMEM((6 * N, N), B16)
WIDE = pltpu.VMEM((2 * H, 6 * N), B16)
ZTAB = pltpu.VMEM((N, 3 * N), B16)
RIGHT = pltpu.VMEM((6 * N, 2 * N), B16)
LEFT = pltpu.VMEM((2 * N, 6 * N), B16)


def planes_of(n):
    return pltpu.VMEM((n, 2, N, N), F32)


def shape(*dims):
    return jax.ShapeDtypeStruct(dims, F32)


def call(body, outs, scratch, *args):
    vmem = pl.BlockSpec(memory_space=pltpu.VMEM)
    return pl.pallas_call(
        body,
        out_shape=outs,
        in_specs=[vmem] * len(args),
        out_specs=jax.tree.map(lambda _: vmem, outs),
        scratch_shapes=scratch,
        compiler_params=pltpu.CompilerParams(vmem_limit_bytes=60 * 2**20),
        name=body.__name__,
    )(*args)


ALL = ("row", "col")


def exchange(data):
    fields = data.shape[0]
    data = data.reshape(fields, H, 8, H)
    data = lax.all_to_all(data, ALL, split_axis=1, concat_axis=1, tiled=True)
    return data.reshape(fields, 8 * H, H)


def shards(base, concentration):
    plain = lax.all_to_all(concentration, "col", split_axis=0, concat_axis=1, tiled=True)
    conc, data = call(
        k1, [shape(2, N, N), shape(2, 8 * H, H)], [pltpu.VMEM((2, N, N), F32), TALL, WIDE, ZTAB, RIGHT], base, plain
    )
    data, conc_hat = call(
        k2,
        [shape(3, 8 * H, H), shape(2 * N, N)],
        [pltpu.VMEM((4, 2 * N, N), F32), TALL, LEFT, LEFT],
        base,
        exchange(data),
    )
    data, before, first = call(
        k3,
        [shape(5, 8 * H, H), shape(6, 2, N, N), shape(ROWS, N)],
        [planes_of(6), pltpu.VMEM((N, 2 * N), F32), TALL, WIDE, ZTAB, ZTAB, RIGHT, RIGHT],
        base,
        exchange(data),
        conc,
    )
    (data,) = call(
        k4,
        [shape(5, 8 * H, H)],
        [pltpu.VMEM((5, 2 * N, N), F32), TALL, LEFT, LEFT],
        base,
        exchange(data),
    )
    data, strain, second = call(
        k5,
        [shape(1, 8 * H, H), shape(6, 2, N, N), shape(ROWS, N)],
        [planes_of(6), pltpu.VMEM((2, N, N), F32), TALL, WIDE, ZTAB, ZTAB, RIGHT, RIGHT],
        base,
        exchange(data),
        conc,
        before,
    )
    sums = lax.psum(jnp.stack([jnp.sum(first), jnp.sum(second)]), ALL)
    strain = lax.all_to_all(strain, "col", split_axis=2, concat_axis=1, tiled=True)
    (data,) = call(
        k6,
        [shape(1, 8 * H, H)],
        [pltpu.VMEM((1, 2 * N, N), F32), TALL, LEFT, LEFT],
        base,
        exchange(data),
        conc_hat,
    )
    (plain,) = call(k7, [shape(2, N, N)], [TALL, WIDE, ZTAB, RIGHT], base, exchange(data))
    result = lax.all_to_all(plain, "col", split_axis=1, concat_axis=0, tiled=True)
    return result, strain, jnp.sqrt(sums * SCALE)


def solution(mesh):
    base = base_tables()
    body = jax.shard_map(
        shards,
        mesh=mesh,
        in_specs=(P(), P("row", "col", None)),
        out_specs=(P("row", "col", None), P(None, "row", "col", None), P()),
        check_vma=False,
    )

    def run(concentration):
        return body(jnp.asarray(base), concentration)

    return run
```

```python
import math

import jax
import jax.numpy as jnp
import numpy as np
from jax import lax
from jax.experimental import pallas as pl
from jax.experimental.pallas import tpu as pltpu
from jax.sharding import PartitionSpec as P

F32 = jnp.float32
B16 = jnp.bfloat16
N = 256
H = 128
ITERS = 2
STEP = 2.0 * math.pi / N
SCALE = 1.0 / float(N) ** 3

FIRST_LOW = 1.0
FIRST_RISE = 0.6
SHEAR_LOW = 0.7
SHEAR_RISE = 0.8
FIRST_REF = 1.3
SHEAR_REF = 1.1
BETA_REF = 2.4 / 3.5
EIGEN_STRAIN = 0.5
WELL_HEIGHT = 1.0
TIME_STEP = 0.5
GRADIENT_ENERGY = 0.5

XX, YY, ZZ, YZ, XZ, XY = range(6)


def base_tables():
    index = np.arange(N)
    angle = (index[:, None] * index[None, :] % N) * (2.0 * np.pi / N)
    parts = []
    for table in (np.cos(angle), np.sin(angle)):
        lead = table.astype(np.float32).astype(jnp.bfloat16)
        rest = (table - lead.astype(np.float64)).astype(np.float32).astype(jnp.bfloat16)
        parts += [lead, rest]
    return np.stack(parts)


def split(value):
    lead = value.astype(B16)
    rest = (value - lead.astype(F32)).astype(B16)
    return lead, rest


def dot(a, b):
    return jnp.dot(a, b, preferred_element_type=F32)


def fill_left(base, out, sine_sign):
    for block, part in enumerate((0, 0, 1)):
        at = block * 2 * N
        cosine, sine = base[part], base[2 + part]
        upper, lower = (sine, -sine) if sine_sign > 0 else (-sine, sine)
        out[0:N, at : at + N] = cosine
        out[0:N, at + N : at + 2 * N] = upper
        out[N : 2 * N, at : at + N] = lower
        out[N : 2 * N, at + N : at + 2 * N] = cosine


def fill_right(base, out, sine_sign):
    for block, part in enumerate((0, 0, 1)):
        at = block * 2 * N
        cosine, sine = base[part], base[2 + part]
        upper, lower = (sine, -sine) if sine_sign > 0 else (-sine, sine)
        out[at : at + N, 0:N] = cosine
        out[at : at + N, N : 2 * N] = upper
        out[at + N : at + 2 * N, 0:N] = lower
        out[at + N : at + 2 * N, N : 2 * N] = cosine


def fill_z_ahead(base, out):
    for block, part in enumerate((0, 0, 1)):
        at = block * N
        out[0:H, at : at + N] = base[part, 0:H, :]
        out[H:N, at : at + N] = -base[2 + part, 0:H, :]


def fill_z_back(base, out):
    column = lax.broadcasted_iota(jnp.int32, (N, H), 1)
    weight = jnp.where(column == 0, 1.0, 2.0)
    for block, part in enumerate((0, 0, 1)):
        at = block * N
        out[:, at : at + H] = (base[part, :, 0:H].astype(F32) * weight).astype(B16)
        out[:, at + H : at + N] = (base[2 + part, :, 0:H].astype(F32) * -weight).astype(B16)


def put_pair(wide, x, real, imag):
    rows = pl.ds(x * H, H)
    for at, value in ((0, real), (N, imag)):
        lead, rest = split(value)
        wide[rows, at : at + N] = lead
        wide[rows, 2 * N + at : 3 * N + at] = rest
        wide[rows, 4 * N + at : 5 * N + at] = lead


def z_ahead(field, z_table, tall, wide, x):
    lead, rest = split(field)
    tall[0:N, :] = lead
    tall[N : 2 * N, :] = rest
    tall[2 * N : 3 * N, :] = lead
    spectrum = dot(z_table[...], tall[0 : 3 * N, :])
    put_pair(wide, x, spectrum[0:H], spectrum[H:N])


def z_back(real, imag, z_table, tall):
    for at, value in ((0, real), (H, imag)):
        lead, rest = split(value)
        tall[at : at + H, :] = lead
        tall[N + at : N + at + H, :] = rest
        tall[2 * N + at : 2 * N + at + H, :] = lead
    return dot(z_table[...], tall[0 : 3 * N, :])


def store_planes(out, field, spectrum):
    for x in range(2):
        for block in range(4):
            out[field, pl.ds(x * 4 + block, H, stride=8), :] = spectrum[
                x * H : (x + 1) * H, block * H : (block + 1) * H
            ]


def load_plane(landed, field, x):
    parts = [landed[field, pl.ds(x * 4 + block, H, stride=8), :] for block in range(4)]
    return jnp.concatenate(parts[0:2], axis=1), jnp.concatenate(parts[2:4], axis=1)


def x_ahead(landed, field, x_table, tall, spectrum, slot):
    for part in range(2):
        for half in range(2):
            rows = landed[field, pl.ds(part * 2 + half, N, stride=4), :]
            lead, rest = split(rows)
            at, lanes = part * N, slice(half * H, (half + 1) * H)
            tall[at : at + N, lanes] = lead
            tall[2 * N + at : 3 * N + at, lanes] = rest
            tall[4 * N + at : 5 * N + at, lanes] = lead
    spectrum[slot] = dot(x_table[...], tall[...])


def x_back(spectrum, slot, x_table, tall, out, field):
    lead, rest = split(spectrum[slot])
    tall[0 : 2 * N, :] = lead
    tall[2 * N : 4 * N, :] = rest
    tall[4 * N : 6 * N, :] = lead
    lines = dot(x_table[...], tall[...])
    for part in range(2):
        for half in range(2):
            out[field, pl.ds(part * 2 + half, N, stride=4), :] = lines[
                part * N : (part + 1) * N, half * H : (half + 1) * H
            ]


def signed(index):
    return jnp.where(index < H, index, index - N).astype(F32) * STEP


def lane_wave(rows, lanes=N):
    return signed(lax.broadcasted_iota(jnp.int32, (rows, lanes), 1))


def row_wave_z():
    return lax.broadcasted_iota(jnp.int32, (H, N), 0).astype(F32) * STEP


CHUNK = 32


def chunk_waves(chunk, kz):
    row = chunk * CHUNK + lax.broadcasted_iota(jnp.int32, (CHUNK, N), 0)
    wave_x = signed(row)
    wave_y = lane_wave(CHUNK)
    wave_z = kz.astype(F32) * STEP
    square = wave_x * wave_x + wave_y * wave_y + wave_z * wave_z
    return wave_x, wave_y, wave_z, square


def green_first(spectrum, source, kz):
    def body(chunk, _):
        wave_x, wave_y, wave_z, square = chunk_waves(chunk, kz)
        nonzero = square > 0.0
        safe = jnp.where(nonzero, square, 1.0)
        factor = jnp.where(nonzero, (BETA_REF - 1.0) * SCALE / (SHEAR_REF * safe), 0.0)
        for part in range(2):
            rows = pl.ds(part * N + chunk * CHUNK, CHUNK)
            psi = spectrum[source, rows, :] * factor
            once = wave_x * psi
            spectrum[0, rows, :] = wave_x * once
            spectrum[1, rows, :] = once
            spectrum[2, rows, :] = psi
        return 0

    lax.fori_loop(0, N // CHUNK, body, 0)


def green_full(spectrum, kz):
    def body(chunk, _):
        wave_x, wave_y, wave_z, square = chunk_waves(chunk, kz)
        nonzero = square > 0.0
        safe = jnp.where(nonzero, square, 1.0)
        scale = jnp.where(nonzero, -SCALE / (SHEAR_REF * safe), 0.0)
        ratio = BETA_REF / safe
        for part in range(2):
            rows = pl.ds(part * N + chunk * CHUNK, CHUNK)
            first, second, third = (spectrum[slot, rows, :] for slot in range(3))
            force_x = wave_x * first + wave_y * second + wave_z * third
            force_y = wave_x * second + spectrum[3, rows, :]
            force_z = wave_x * third + spectrum[4, rows, :]
            along = (wave_x * force_x + wave_y * force_y + wave_z * force_z) * ratio
            moved_x = scale * (force_x - along * wave_x)
            moved_y = scale * (force_y - along * wave_y)
            moved_z = scale * (force_z - along * wave_z)
            spectrum[0, rows, :] = wave_x * moved_x
            spectrum[1, rows, :] = 0.5 * (wave_x * moved_y + wave_y * moved_x)
            spectrum[2, rows, :] = 0.5 * (wave_x * moved_z + wave_z * moved_x)
            spectrum[3, rows, :] = moved_y
            spectrum[4, rows, :] = moved_z
        return 0

    lax.fori_loop(0, N // CHUNK, body, 0)


def relax(spectrum, drive, conc, kz):
    def body(chunk, _):
        _, _, _, square = chunk_waves(chunk, kz)
        inverse = SCALE / (1.0 + TIME_STEP * GRADIENT_ENERGY * square * square)
        for part in range(2):
            rows = pl.ds(part * N + chunk * CHUNK, CHUNK)
            value = conc[rows, :] - TIME_STEP * square * spectrum[drive, rows, :]
            spectrum[drive, rows, :] = value * inverse
        return 0

    lax.fori_loop(0, N // CHUNK, body, 0)


ROWS = 32


def eigen_stress(conc):
    rise = (3.0 * FIRST_RISE + 2.0 * SHEAR_RISE) * EIGEN_STRAIN
    low = (3.0 * FIRST_LOW + 2.0 * SHEAR_LOW) * EIGEN_STRAIN
    return (0.5 - conc) * (rise * (conc + 0.5) + low)


def polarize(parts, conc):
    first = FIRST_LOW + FIRST_RISE * conc
    excess = 2.0 * (SHEAR_LOW + SHEAR_RISE * conc - SHEAR_REF)
    normal = (first - FIRST_REF) * (parts[0] + parts[1] + parts[2]) + eigen_stress(conc)
    return [normal + excess * p for p in parts[:3]] + [excess * p for p in parts[3:]]


def potential(parts, conc):
    first = FIRST_LOW + FIRST_RISE * conc
    shear = SHEAR_LOW + SHEAR_RISE * conc
    dilation = EIGEN_STRAIN * conc
    d = [p - dilation for p in parts[:3]]
    trace = d[0] + d[1] + d[2]
    energy = d[0] * d[0] + d[1] * d[1] + d[2] * d[2]
    energy = energy + 2.0 * (parts[3] * parts[3] + parts[4] * parts[4] + parts[5] * parts[5])
    chemical = 2.0 * WELL_HEIGHT * conc * (1.0 - conc) * (1.0 - 2.0 * conc)
    return (
        chemical
        + 0.5 * FIRST_RISE * trace * trace
        + SHEAR_RISE * energy
        - EIGEN_STRAIN * (3.0 * first + 2.0 * shear) * trace
    )


def sum_squares(parts):
    total = parts[0] * parts[0]
    for part in parts[1:]:
        total = total + part * part
    return total


def fold(value):
    tile = value[0:8, 0:H] + value[0:8, H:N]
    for at in range(8, ROWS, 8):
        tile = tile + (value[at : at + 8, 0:H] + value[at : at + 8, H:N])
    return tile


ORDER = (XX, XY, XZ, YY, YZ, ZZ)
PRESSURE, CONC, FIRST, STRESS, SHIFT, DRIVE, NEXT = 0, 1, 2, 5, 10, 15, 16
FIELDS = 17
COLS, LINES = 16, 8
MESH = pl.DeviceIdType.MESH


def step_kernel(
    base,
    concentration,
    result,
    strain_out,
    norms,
    landed,
    sent,
    plain,
    conc,
    work,
    before,
    turned,
    spectrum,
    conc_hat,
    planes,
    lines,
    tall,
    wide,
    zf,
    zb,
    yf,
    yb,
    xf,
    xb,
    partial,
    col_sums,
    row_sums,
    send_sems,
    recv_sems,
    side_send,
    side_recv,
):
    row, col = lax.axis_index("row"), lax.axis_index("col")
    me = row * COLS + col
    next_col = lax.rem(col + 1, COLS)

    def tiles(ref, field, device):
        return ref.at[field, pl.ds(pl.multiple_of(device * 8, 8), 8), :]

    def send(field):
        def go(i, _):
            other = lax.rem(me + i, 128)
            pltpu.make_async_remote_copy(
                src_ref=tiles(sent, field, other),
                dst_ref=tiles(landed, field, me),
                send_sem=send_sems.at[field],
                recv_sem=recv_sems.at[field],
                device_id=(other // COLS, lax.rem(other, COLS)),
                device_id_type=MESH,
            ).start()
            return 0

        lax.fori_loop(1, 128, go, 0)
        own = pl.ds(pl.multiple_of(me * 8, 8), 8)
        landed[field, own, :] = sent[field, own, :]

    def whole(field):
        rows = pl.ds(0, 127 * 8)
        return pltpu.make_async_remote_copy(
            src_ref=sent.at[field, rows, :],
            dst_ref=landed.at[field, rows, :],
            send_sem=send_sems.at[field],
            recv_sem=recv_sems.at[field],
            device_id=(row, next_col),
            device_id_type=MESH,
        )

    def receive(field):
        whole(field).wait_recv()

    def column_copy(src_of, dst, index, target):
        return pltpu.make_async_remote_copy(
            src_ref=src_of(target),
            dst_ref=dst,
            send_sem=side_send.at[index],
            recv_sem=side_recv.at[index],
            device_id=(row, target),
            device_id_type=MESH,
        )

    def column_send(src_of, dst, index):
        def go(i, _):
            column_copy(src_of, dst, index, lax.rem(col + i, COLS)).start()
            return 0

        lax.fori_loop(1, COLS, go, 0)

    def lines_of(device):
        return pl.ds(pl.multiple_of(device * 16, 16), 16)

    def pair_of(device):
        return pl.ds(device * 2, 2)

    column_send(lambda t: concentration.at[pair_of(t)], plain.at[:, lines_of(col), :], 0)
    plain[:, lines_of(col), :] = concentration[pair_of(col)]
    fill_z_ahead(base, zf)
    fill_z_back(base, zb)
    fill_right(base, yf, -1)
    fill_right(base, yb, 1)
    fill_left(base, xf, 1)
    fill_left(base, xb, -1)

    def arrived(src, dst, index):
        return pltpu.make_async_remote_copy(
            src_ref=src,
            dst_ref=dst,
            send_sem=side_send.at[index],
            recv_sem=side_recv.at[index],
            device_id=(row, next_col),
            device_id_type=MESH,
        )

    arrived(concentration.at[pl.ds(0, 30)], plain.at[:, pl.ds(0, 240), :], 0).wait_recv()
    for x in range(2):
        conc[x] = plain[x].T

    def first_ahead(k, _):
        def choose(chunk, _):
            rows = pl.ds(chunk * ROWS, ROWS)
            for x in range(2):
                value = conc[x, rows, :]
                work[0, x, rows, :] = jnp.where(k == 0, eigen_stress(value), value)
            return 0

        lax.fori_loop(0, N // ROWS, choose, 0)
        ahead(0)
        store_planes(sent, PRESSURE + k, lines)
        send(PRESSURE + k)
        return 0

    def ahead(slot):
        for x in range(2):
            z_ahead(work[slot, x], zf, tall, wide, x)
        lines[...] = dot(wide[...], yf[...])

    lax.fori_loop(0, 2, first_ahead, 0)

    receive(PRESSURE)
    x_ahead(landed, PRESSURE, xf, tall, spectrum, 3)
    green_first(spectrum, 3, me)

    def first_back(slot, _):
        x_back(spectrum, slot, xb, tall, sent, FIRST + slot)
        send(FIRST + slot)
        return 0

    lax.fori_loop(0, 3, first_back, 0)
    receive(CONC)
    x_ahead(landed, CONC, xf, tall, spectrum, 3)
    conc_hat[...] = spectrum[3]

    wave_y, wave_z = lane_wave(H), row_wave_z()

    def put(x, real, imag, factor=None):
        if factor is not None:
            real, imag = factor * real, factor * imag
        put_pair(wide, x, real, imag)

    def back(slot):
        lines[...] = dot(wide[...], yb[...])
        for x in range(2):
            rows = slice(x * H, (x + 1) * H)
            work[slot, x] = z_back(lines[rows, 0:N], lines[rows, N : 2 * N], zb, tall)

    def first_strain(k, _):
        for slot, field, factor in (
            (0, 0, None),
            (1, 1, wave_y),
            (2, 1, wave_z),
            (3, 2, wave_y * wave_y),
            (4, 2, wave_y * wave_z),
            (5, 2, wave_z * wave_z),
        ):

            @pl.when(k == slot)
            def _():
                if slot in (0, 1, 3):
                    receive(FIRST + field)
                for x in range(2):
                    put(x, *load_plane(landed, FIRST + field, x), factor)

        back(k)
        return 0

    lax.fori_loop(0, 6, first_strain, 0)
    partial[...] = jnp.zeros_like(partial)

    def stress(chunk, _):
        rows = pl.ds(chunk * ROWS, ROWS)
        for x in range(2):
            parts = [work[i, x, rows, :] for i in range(6)]
            for i in range(6):
                before[i, x, rows, :] = parts[i]
            partial[0] += sum_squares(parts)
            xx, xy, xz, yy, yz, zz = parts
            value = polarize([xx, yy, zz, yz, xz, xy], conc[x, rows, :])
            for i, which in enumerate(ORDER):
                work[i, x, rows, :] = value[which]
        return 0

    lax.fori_loop(0, N // ROWS, stress, 0)

    def stress_ahead(k, _):
        ahead(k)

        @pl.when(k >= 3)
        def _():
            def mix(chunk, _):
                rows = pl.ds(chunk * ROWS, ROWS)
                index = chunk * ROWS + lax.broadcasted_iota(jnp.int32, (ROWS, N), 0)
                along_z = jnp.where(index < H, index, index - H).astype(F32) * STEP
                along_y = lane_wave(ROWS)
                for part in range(2):
                    lanes = slice(part * N, (part + 1) * N)
                    value = lines[rows, lanes]
                    lines[rows, lanes] = planes[rows, lanes] + along_z * value
                    planes[rows, lanes] = along_y * value
                return 0

            lax.fori_loop(0, N // ROWS, mix, 0)

        @pl.when(k != 3)
        def _():
            field = STRESS + jnp.where(k < 3, k, k - 1)
            store_planes(sent, field, lines)
            send(field)

        return 0

    planes[...] = jnp.zeros_like(planes)
    lax.fori_loop(0, 6, stress_ahead, 0)

    def stress_x(slot, _):
        receive(STRESS + slot)
        x_ahead(landed, STRESS + slot, xf, tall, spectrum, slot)
        return 0

    lax.fori_loop(0, 5, stress_x, 0)
    green_full(spectrum, me)

    def shift_x(slot, _):
        x_back(spectrum, slot, xb, tall, sent, SHIFT + slot)
        send(SHIFT + slot)
        return 0

    lax.fori_loop(0, 5, shift_x, 0)

    def second_strain(k, _):
        for slot, field, factor in (
            (0, 0, None),
            (1, 1, None),
            (2, 2, None),
            (3, 3, wave_y),
            (5, 4, wave_z),
        ):

            @pl.when(k == slot)
            def _():
                if slot < 4:
                    receive(SHIFT + field)
                for x in range(2):
                    put(x, *load_plane(landed, SHIFT + field, x), factor)

        @pl.when(k == 4)
        def _():
            receive(SHIFT + 4)
            for x in range(2):
                real_y, imag_y = load_plane(landed, SHIFT + 3, x)
                real_z, imag_z = load_plane(landed, SHIFT + 4, x)
                put(
                    x,
                    0.5 * (wave_y * real_z + wave_z * real_y),
                    0.5 * (wave_y * imag_z + wave_z * imag_y),
                )

        back(k)
        for x in range(2):
            turned[k, x] = work[k, x].T
        return 0

    lax.fori_loop(0, 6, second_strain, 0)

    def drive(chunk, _):
        rows = pl.ds(chunk * ROWS, ROWS)
        for x in range(2):
            parts = [work[i, x, rows, :] for i in range(6)]
            partial[1] += sum_squares([p - before[i, x, rows, :] for i, p in enumerate(parts)])
            xx, xy, xz, yy, yz, zz = parts
            work[0, x, rows, :] = potential([xx, yy, zz, yz, xz, xy], conc[x, rows, :])
        return 0

    lax.fori_loop(0, N // ROWS, drive, 0)
    ahead(0)
    store_planes(sent, DRIVE, lines)
    send(DRIVE)

    def strain_send(slots):
        for slot in slots:
            column_send(
                lambda t: turned.at[slot, :, lines_of(t), :],
                strain_out.at[ORDER[slot], pair_of(col)],
                1 + slot,
            )
            own = pltpu.make_async_copy(
                turned.at[slot, :, lines_of(col), :],
                strain_out.at[ORDER[slot], pair_of(col)],
                side_send.at[9 + slot],
            )
            own.start()

    col_sums[col, 0:8, :] = fold(partial[0])
    col_sums[col, 8:16, :] = fold(partial[1])
    column_send(lambda t: col_sums.at[col], col_sums.at[col], 8)
    strain_send((0, 1))

    receive(DRIVE)
    x_ahead(landed, DRIVE, xf, tall, spectrum, 0)
    relax(spectrum, 0, conc_hat, me)
    x_back(spectrum, 0, xb, tall, sent, NEXT)
    send(NEXT)
    strain_send((2, 3))

    arrived(col_sums.at[pl.ds(0, 15)], col_sums.at[pl.ds(0, 15)], 8).wait_recv()
    total = col_sums[0]
    for i in range(1, COLS):
        total = total + col_sums[i]
    row_sums[row] = total

    def row_send(i, _):
        pltpu.make_async_remote_copy(
            src_ref=row_sums.at[row],
            dst_ref=row_sums.at[row],
            send_sem=side_send.at[15],
            recv_sem=side_recv.at[15],
            device_id=(lax.rem(row + i, LINES), col),
            device_id_type=MESH,
        ).start()
        return 0

    lax.fori_loop(1, LINES, row_send, 0)

    receive(NEXT)
    for x in range(2):
        put(x, *load_plane(landed, NEXT, x))
    back(0)
    for x in range(2):
        work[1, x] = work[0, x].T
    column_send(lambda t: work.at[1, :, lines_of(t), :], result.at[pair_of(col)], 7)
    own = pltpu.make_async_copy(
        work.at[1, :, lines_of(col), :], result.at[pair_of(col)], side_send.at[16]
    )
    own.start()
    strain_send((4, 5))

    row_wait = pltpu.make_async_remote_copy(
        src_ref=row_sums.at[pl.ds(0, LINES - 1)],
        dst_ref=row_sums.at[pl.ds(0, LINES - 1)],
        send_sem=side_send.at[15],
        recv_sem=side_recv.at[15],
        device_id=(lax.rem(row + 1, LINES), col),
        device_id_type=MESH,
    )
    row_wait.wait_recv()
    total = row_sums[0]
    for i in range(1, LINES):
        total = total + row_sums[i]
    norms[...] = total
    row_wait.wait_send()

    def sent_all(field, _):
        whole(field).wait_send()
        return 0

    lax.fori_loop(0, FIELDS, sent_all, 0)
    arrived(concentration.at[pl.ds(0, 30)], plain.at[:, pl.ds(0, 240), :], 0).wait_send()
    arrived(col_sums.at[pl.ds(0, 15)], col_sums.at[pl.ds(0, 15)], 8).wait_send()
    for slot in range(6):
        both = arrived(turned.at[slot, :, pl.ds(0, 240), :], strain_out.at[ORDER[slot], pl.ds(0, 30)], 1 + slot)
        both.wait_send()
        both.wait_recv()
        pltpu.make_async_copy(
            turned.at[slot, :, lines_of(col), :],
            strain_out.at[ORDER[slot], pair_of(col)],
            side_send.at[9 + slot],
        ).wait()
    both = arrived(work.at[1, :, pl.ds(0, 240), :], result.at[pl.ds(0, 30)], 7)
    both.wait_send()
    both.wait_recv()
    own.wait()


def shape(*dims):
    return jax.ShapeDtypeStruct(dims, F32)


def shards(base, concentration):
    vmem = pl.BlockSpec(memory_space=pltpu.VMEM)
    hbm = pl.BlockSpec(memory_space=pl.ANY)
    result, strain, norms = pl.pallas_call(
        step_kernel,
        out_shape=[shape(32, 16, N), shape(6, 32, 16, N), shape(16, H)],
        in_specs=[vmem, vmem],
        out_specs=[hbm, hbm, vmem],
        scratch_shapes=[
            pltpu.VMEM((FIELDS, 8 * H, H), F32),
            pltpu.VMEM((FIELDS, 8 * H, H), F32),
            pltpu.VMEM((2, N, N), F32),
            pltpu.VMEM((2, N, N), F32),
            pltpu.VMEM((6, 2, N, N), F32),
            pltpu.VMEM((6, 2, N, N), F32),
            pltpu.VMEM((6, 2, N, N), F32),
            pltpu.VMEM((5, 2 * N, N), F32),
            pltpu.VMEM((2 * N, N), F32),
            pltpu.VMEM((N, 2 * N), F32),
            pltpu.VMEM((N, 2 * N), F32),
            pltpu.VMEM((6 * N, N), B16),
            pltpu.VMEM((2 * H, 6 * N), B16),
            pltpu.VMEM((N, 3 * N), B16),
            pltpu.VMEM((N, 3 * N), B16),
            pltpu.VMEM((6 * N, 2 * N), B16),
            pltpu.VMEM((6 * N, 2 * N), B16),
            pltpu.VMEM((2 * N, 6 * N), B16),
            pltpu.VMEM((2 * N, 6 * N), B16),
            pltpu.VMEM((2, ROWS, N), F32),
            pltpu.VMEM((COLS, 16, H), F32),
            pltpu.VMEM((LINES, 16, H), F32),
            pltpu.SemaphoreType.DMA((FIELDS,)),
            pltpu.SemaphoreType.DMA((FIELDS,)),
            pltpu.SemaphoreType.DMA((17,)),
            pltpu.SemaphoreType.DMA((17,)),
        ],
        compiler_params=pltpu.CompilerParams(
            vmem_limit_bytes=60 * 2**20, has_side_effects=True
        ),
        name="step",
    )(base, concentration)
    sums = jnp.sum(norms.reshape(2, 8 * H), axis=1)
    return result, strain, jnp.sqrt(sums * SCALE)


def solution(mesh):
    base = base_tables()
    body = jax.shard_map(
        shards,
        mesh=mesh,
        in_specs=(P(), P("row", "col", None)),
        out_specs=(P("row", "col", None), P(None, "row", "col", None), P()),
        check_vma=False,
    )

    def run(concentration):
        return body(jnp.asarray(base), concentration)

    return run
```

```python
import math

import jax
import jax.numpy as jnp
import numpy as np
from jax import lax
from jax.experimental import pallas as pl
from jax.experimental.pallas import tpu as pltpu
from jax.sharding import PartitionSpec as P

F32 = jnp.float32
B16 = jnp.bfloat16
N = 256
H = 128
ITERS = 2
STEP = 2.0 * math.pi / N
SCALE = 1.0 / float(N) ** 3

FIRST_LOW = 1.0
FIRST_RISE = 0.6
SHEAR_LOW = 0.7
SHEAR_RISE = 0.8
FIRST_REF = 1.3
SHEAR_REF = 1.1
BETA_REF = 2.4 / 3.5
EIGEN_STRAIN = 0.5
WELL_HEIGHT = 1.0
TIME_STEP = 0.5
GRADIENT_ENERGY = 0.5

XX, YY, ZZ, YZ, XZ, XY = range(6)


def base_tables():
    index = np.arange(N)
    angle = (index[:, None] * index[None, :] % N) * (2.0 * np.pi / N)
    parts = []
    for table in (np.cos(angle), np.sin(angle)):
        lead = table.astype(np.float32).astype(jnp.bfloat16)
        rest = (table - lead.astype(np.float64)).astype(np.float32).astype(jnp.bfloat16)
        parts += [lead, rest]
    return np.stack(parts)


def split(value):
    lead = value.astype(B16)
    rest = (value - lead.astype(F32)).astype(B16)
    return lead, rest


def dot(a, b):
    return jnp.dot(a, b, preferred_element_type=F32)


def fill_left(base, out, sine_sign):
    for block, part in enumerate((0, 0, 1)):
        at = block * 2 * N
        cosine, sine = base[part], base[2 + part]
        upper, lower = (sine, -sine) if sine_sign > 0 else (-sine, sine)
        out[0:N, at : at + N] = cosine
        out[0:N, at + N : at + 2 * N] = upper
        out[N : 2 * N, at : at + N] = lower
        out[N : 2 * N, at + N : at + 2 * N] = cosine


def fill_right(base, out, sine_sign):
    for block, part in enumerate((0, 0, 1)):
        at = block * 2 * N
        cosine, sine = base[part], base[2 + part]
        upper, lower = (sine, -sine) if sine_sign > 0 else (-sine, sine)
        out[at : at + N, 0:N] = cosine
        out[at : at + N, N : 2 * N] = upper
        out[at + N : at + 2 * N, 0:N] = lower
        out[at + N : at + 2 * N, N : 2 * N] = cosine


def fill_z_ahead(base, out):
    for block, part in enumerate((0, 0, 1)):
        at = block * N
        out[0:H, at : at + N] = base[part, 0:H, :]
        out[H:N, at : at + N] = -base[2 + part, 0:H, :]


def fill_z_back(base, out):
    column = lax.broadcasted_iota(jnp.int32, (N, H), 1)
    weight = jnp.where(column == 0, 1.0, 2.0)
    for block, part in enumerate((0, 0, 1)):
        at = block * N
        out[:, at : at + H] = (base[part, :, 0:H].astype(F32) * weight).astype(B16)
        out[:, at + H : at + N] = (base[2 + part, :, 0:H].astype(F32) * -weight).astype(B16)


def put_pair(wide, x, real, imag):
    rows = pl.ds(x * H, H)
    for at, value in ((0, real), (N, imag)):
        lead, rest = split(value)
        wide[rows, at : at + N] = lead
        wide[rows, 2 * N + at : 3 * N + at] = rest
        wide[rows, 4 * N + at : 5 * N + at] = lead


def z_ahead(field, z_table, tall):
    lead, rest = split(field)
    tall[0:N, :] = lead
    tall[N : 2 * N, :] = rest
    tall[2 * N : 3 * N, :] = lead
    return dot(z_table[...], tall[0 : 3 * N, :])


def z_back(real, imag, z_table, tall):
    for at, value in ((0, real), (H, imag)):
        lead, rest = split(value)
        tall[at : at + H, :] = lead
        tall[N + at : N + at + H, :] = rest
        tall[2 * N + at : 2 * N + at + H, :] = lead
    return dot(z_table[...], tall[0 : 3 * N, :])


def store_planes(out, field, spectrum):
    for x in range(2):
        for block in range(4):
            out[field, pl.ds(x * 4 + block, H, stride=8), :] = spectrum[
                x * H : (x + 1) * H, block * H : (block + 1) * H
            ]


def load_plane(landed, field, x):
    parts = [landed[field, pl.ds(x * 4 + block, H, stride=8), :] for block in range(4)]
    return jnp.concatenate(parts[0:2], axis=1), jnp.concatenate(parts[2:4], axis=1)


def put_tall(tall, part, rows, lanes):
    lead, rest = split(rows)
    at = part * N
    tall[at : at + N, lanes] = lead
    tall[2 * N + at : 3 * N + at, lanes] = rest
    tall[4 * N + at : 5 * N + at, lanes] = lead


def x_ahead(landed, field, x_table, tall, spectrum, slot):
    for part in range(2):
        for half in range(2):
            rows = landed[field, pl.ds(part * 2 + half, N, stride=4), :]
            put_tall(tall, part, rows, slice(half * H, (half + 1) * H))
    spectrum[slot] = dot(x_table[...], tall[...])


def x_lines(source, x_table, tall):
    for part in range(2):
        put_tall(tall, part, source[part * N : (part + 1) * N], slice(0, N))
    return dot(x_table[...], tall[...])


def store_lines(out, field, lines):
    for part in range(2):
        for half in range(2):
            out[field, pl.ds(part * 2 + half, N, stride=4), :] = lines[
                part * N : (part + 1) * N, half * H : (half + 1) * H
            ]


def put_rows(wide, rows, at, value):
    lead, rest = split(value)
    count = value.shape[1]
    wide[rows, at : at + count] = lead
    wide[rows, 2 * N + at : 2 * N + at + count] = rest
    wide[rows, 4 * N + at : 4 * N + at + count] = lead


def turn_groups(value):
    row = lax.broadcasted_iota(jnp.int32, value.shape, 1)
    group = lax.broadcasted_iota(jnp.int32, value.shape, 2) // 16
    for bit in (1, 2, 4):
        row_set, group_set = (row & bit) != 0, (group & bit) != 0
        above = pltpu.roll(pltpu.roll(value, 8 - bit, axis=1), 16 * bit, axis=2)
        below = pltpu.roll(pltpu.roll(value, bit, axis=1), H - 16 * bit, axis=2)
        value = jnp.where(row_set == group_set, value, jnp.where(group_set, above, below))
    return value


def tile_rows(block, part, high, which):
    return pl.ds(block * H + high * 64 + part * 4 + which, 8, stride=8)


def gather_cells(landed, field, wide):
    def go(block, _):
        for part in range(2):
            for high in range(2):
                parts = [landed[field, tile_rows(block, part, high, i), :] for i in range(4)]
                value = turn_groups(jnp.stack(parts)).reshape(32, H)
                put_rows(wide, pl.ds(block * 32, 32), part * N + high * H, value)
        return 0

    lax.fori_loop(0, 8, go, 0)


def scatter_cells(out, field, lines):
    def go(block, _):
        for part in range(2):
            for high in range(2):
                at = part * N + high * H
                value = lines[pl.ds(block * 32, 32), at : at + H].reshape(4, 8, H)
                value = turn_groups(value)
                for i in range(4):
                    out[field, tile_rows(block, part, high, i), :] = value[i]
        return 0

    lax.fori_loop(0, 8, go, 0)


def signed(index):
    return jnp.where(index < H, index, index - N).astype(F32) * STEP


def lane_wave(rows, lanes=N):
    return signed(lax.broadcasted_iota(jnp.int32, (rows, lanes), 1))


def row_wave_z():
    return lax.broadcasted_iota(jnp.int32, (H, N), 0).astype(F32) * STEP


CHUNK = 32


def chunk_waves(chunk, kz):
    row = chunk * CHUNK + lax.broadcasted_iota(jnp.int32, (CHUNK, N), 0)
    wave_x = signed(row)
    wave_y = lane_wave(CHUNK)
    wave_z = kz.astype(F32) * STEP
    square = wave_x * wave_x + wave_y * wave_y + wave_z * wave_z
    return wave_x, wave_y, wave_z, square


def green_first(spectrum, source, kz):
    def body(chunk, _):
        wave_x, wave_y, wave_z, square = chunk_waves(chunk, kz)
        nonzero = square > 0.0
        safe = jnp.where(nonzero, square, 1.0)
        factor = jnp.where(nonzero, (BETA_REF - 1.0) * SCALE / (SHEAR_REF * safe), 0.0)
        for part in range(2):
            rows = pl.ds(part * N + chunk * CHUNK, CHUNK)
            psi = spectrum[source, rows, :] * factor
            once = wave_x * psi
            spectrum[0, rows, :] = wave_x * once
            spectrum[1, rows, :] = once
            spectrum[2, rows, :] = psi
        return 0

    lax.fori_loop(0, N // CHUNK, body, 0)


def green_full(spectrum, kz):
    def body(chunk, _):
        wave_x, wave_y, wave_z, square = chunk_waves(chunk, kz)
        nonzero = square > 0.0
        safe = jnp.where(nonzero, square, 1.0)
        scale = jnp.where(nonzero, -SCALE / (SHEAR_REF * safe), 0.0)
        ratio = BETA_REF / safe
        for part in range(2):
            rows = pl.ds(part * N + chunk * CHUNK, CHUNK)
            first, second, third = (spectrum[slot, rows, :] for slot in range(3))
            force_x = wave_x * first + wave_y * second + wave_z * third
            force_y = wave_x * second + spectrum[3, rows, :]
            force_z = wave_x * third + spectrum[4, rows, :]
            along = (wave_x * force_x + wave_y * force_y + wave_z * force_z) * ratio
            moved_x = scale * (force_x - along * wave_x)
            moved_y = scale * (force_y - along * wave_y)
            moved_z = scale * (force_z - along * wave_z)
            spectrum[XX, rows, :] = wave_x * moved_x
            spectrum[YY, rows, :] = wave_y * moved_y
            spectrum[ZZ, rows, :] = wave_z * moved_z
            spectrum[YZ, rows, :] = 0.5 * (wave_y * moved_z + wave_z * moved_y)
            spectrum[XZ, rows, :] = 0.5 * (wave_x * moved_z + wave_z * moved_x)
            spectrum[XY, rows, :] = 0.5 * (wave_x * moved_y + wave_y * moved_x)
        return 0

    lax.fori_loop(0, N // CHUNK, body, 0)


def relax(spectrum, drive, conc, kz):
    def body(chunk, _):
        _, _, _, square = chunk_waves(chunk, kz)
        inverse = SCALE / (1.0 + TIME_STEP * GRADIENT_ENERGY * square * square)
        for part in range(2):
            rows = pl.ds(part * N + chunk * CHUNK, CHUNK)
            value = conc[rows, :] - TIME_STEP * square * spectrum[drive, rows, :]
            spectrum[drive, rows, :] = value * inverse
        return 0

    lax.fori_loop(0, N // CHUNK, body, 0)


ROWS = 32


def eigen_stress(conc):
    rise = (3.0 * FIRST_RISE + 2.0 * SHEAR_RISE) * EIGEN_STRAIN
    low = (3.0 * FIRST_LOW + 2.0 * SHEAR_LOW) * EIGEN_STRAIN
    return (0.5 - conc) * (rise * (conc + 0.5) + low)


def polarize(parts, conc):
    first = FIRST_LOW + FIRST_RISE * conc
    excess = 2.0 * (SHEAR_LOW + SHEAR_RISE * conc - SHEAR_REF)
    normal = (first - FIRST_REF) * (parts[0] + parts[1] + parts[2]) + eigen_stress(conc)
    return [normal + excess * p for p in parts[:3]] + [excess * p for p in parts[3:]]


def potential(parts, conc):
    first = FIRST_LOW + FIRST_RISE * conc
    shear = SHEAR_LOW + SHEAR_RISE * conc
    dilation = EIGEN_STRAIN * conc
    d = [p - dilation for p in parts[:3]]
    trace = d[0] + d[1] + d[2]
    energy = d[0] * d[0] + d[1] * d[1] + d[2] * d[2]
    energy = energy + 2.0 * (parts[3] * parts[3] + parts[4] * parts[4] + parts[5] * parts[5])
    chemical = 2.0 * WELL_HEIGHT * conc * (1.0 - conc) * (1.0 - 2.0 * conc)
    return (
        chemical
        + 0.5 * FIRST_RISE * trace * trace
        + SHEAR_RISE * energy
        - EIGEN_STRAIN * (3.0 * first + 2.0 * shear) * trace
    )


def sum_squares(parts):
    total = parts[0] * parts[0]
    for part in parts[1:]:
        total = total + part * part
    return total


def fold(value):
    tile = value[0:8, 0:H] + value[0:8, H:N]
    for at in range(8, ROWS, 8):
        tile = tile + (value[at : at + 8, 0:H] + value[at : at + 8, H:N])
    return tile


ORDER = (XX, XY, XZ, YY, YZ, ZZ)
PRESSURE, CONC, FIRST, STRESS, SHIFT, DRIVE, NEXT = 0, 1, 2, 5, 10, 16, 17
FIELDS = 18
COLS, LINES = 16, 8
MESH = pl.DeviceIdType.MESH


def step_kernel(
    base,
    concentration,
    result,
    strain_out,
    norms,
    landed,
    sent,
    plain,
    cells,
    conc,
    work,
    before,
    kept,
    turned,
    spectrum,
    conc_hat,
    planes,
    lines,
    tall,
    wide,
    zf,
    zb,
    yf,
    yb,
    xf,
    xb,
    partial,
    col_sums,
    row_sums,
    send_sems,
    recv_sems,
    side_send,
    side_recv,
):
    row, col = lax.axis_index("row"), lax.axis_index("col")
    me = row * COLS + col
    next_col = lax.rem(col + 1, COLS)

    def tiles(ref, field, device):
        return ref.at[field, pl.ds(pl.multiple_of(device * 8, 8), 8), :]

    def send(field):
        def go(i, _):
            other = lax.rem(me + i, 128)
            pltpu.make_async_remote_copy(
                src_ref=tiles(sent, field, other),
                dst_ref=tiles(landed, field, me),
                send_sem=send_sems.at[field],
                recv_sem=recv_sems.at[field],
                device_id=(other // COLS, lax.rem(other, COLS)),
                device_id_type=MESH,
            ).start()
            return 0

        lax.fori_loop(1, 128, go, 0)
        own = pl.ds(pl.multiple_of(me * 8, 8), 8)
        landed[field, own, :] = sent[field, own, :]

    def whole(field):
        rows = pl.ds(0, 127 * 8)
        return pltpu.make_async_remote_copy(
            src_ref=sent.at[field, rows, :],
            dst_ref=landed.at[field, rows, :],
            send_sem=send_sems.at[field],
            recv_sem=recv_sems.at[field],
            device_id=(row, next_col),
            device_id_type=MESH,
        )

    def receive(field):
        whole(field).wait_recv()

    def side_copy(src, dst, index, device):
        return pltpu.make_async_remote_copy(
            src_ref=src,
            dst_ref=dst,
            send_sem=side_send.at[index],
            recv_sem=side_recv.at[index],
            device_id=device,
            device_id_type=MESH,
        )

    def column_send(src_of, dst, index):
        def go(i, _):
            target = lax.rem(col + i, COLS)
            side_copy(src_of(target), dst, index, (row, target)).start()
            return 0

        lax.fori_loop(1, COLS, go, 0)

    def lines_of(device):
        return pl.ds(pl.multiple_of(device * 16, 16), 16)

    def pair_of(device):
        return pl.ds(device * 2, 2)


    def cells_ahead(field, field_of):
        for half in range(2):
            value = z_ahead(field_of(half), zf, tall)
            for part in range(2):
                for j in range(2):
                    sent[field, pl.ds(part * 4 + 2 * half + j, H, stride=8), :] = value[
                        part * H : (part + 1) * H, j * H : (j + 1) * H
                    ]

    def cells_back(field, half):
        parts = [landed[field, pl.ds(i, H, stride=8), :] for i in range(8)]
        real = jnp.concatenate(parts[2 * half : 2 * half + 2], axis=1)
        imag = jnp.concatenate(parts[4 + 2 * half : 6 + 2 * half], axis=1)
        return z_back(real, imag, zb, tall)

    def plane_ahead(field, slot):
        gather_cells(landed, field, wide)
        lines[...] = dot(wide[...], yf[...])
        for part in range(2):
            put_tall(tall, part, lines[:, part * N : (part + 1) * N], slice(0, N))
        spectrum[slot] = dot(xf[...], tall[...])

    def plane_lines(value, factor=None):
        for part in range(2):
            rows = value[part * N : (part + 1) * N]
            if factor is not None:
                rows = factor * rows
            put_rows(wide, slice(0, N), part * N, rows)

    def plane_back():
        lines[...] = dot(wide[...], yb[...])

    fill_z_ahead(base, zf)
    for half in range(2):
        block = concentration[16 * half : 16 * half + 16].reshape(N, N)
        cells[half] = block.T

    def first_pressure(half):
        return eigen_stress(cells[half])

    cells_ahead(PRESSURE, first_pressure)
    send(PRESSURE)
    column_send(lambda t: concentration.at[pair_of(t)], plain.at[:, lines_of(col), :], 0)
    plain[:, lines_of(col), :] = concentration[pair_of(col)]
    plain_src, plain_dst = concentration.at[pl.ds(0, 30)], plain.at[:, pl.ds(0, 240), :]
    plain_wait = side_copy(plain_src, plain_dst, 0, (row, next_col))
    fill_right(base, yf, -1)
    fill_left(base, xf, 1)
    fill_left(base, xb, -1)
    fill_z_back(base, zb)
    fill_right(base, yb, 1)
    cells_ahead(CONC, lambda half: cells[half])

    receive(PRESSURE)
    plane_ahead(PRESSURE, 3)
    green_first(spectrum, 3, me)

    def first_back(slot, _):
        kept[slot] = x_lines(spectrum.at[slot], xb, tall)
        store_lines(sent, FIRST + slot, kept.at[slot])
        send(FIRST + slot)
        return 0

    lax.fori_loop(0, 3, first_back, 0)
    send(CONC)
    plain_wait.wait_recv()
    for x in range(2):
        conc[x] = plain[x].T

    wave_y, wave_z = lane_wave(H), row_wave_z()

    def first_strain(k, _):
        for slot, field, factor in (
            (0, 0, None),
            (1, 1, wave_y),
            (2, 1, wave_z),
            (3, 2, wave_y * wave_y),
            (4, 2, wave_y * wave_z),
            (5, 2, wave_z * wave_z),
        ):

            @pl.when(k == slot)
            def _():
                if slot in (0, 1, 3):
                    receive(FIRST + field)
                for x in range(2):
                    real, imag = load_plane(landed, FIRST + field, x)
                    if factor is not None:
                        real, imag = factor * real, factor * imag
                    put_pair(wide, x, real, imag)

        plane_back()
        for x in range(2):
            rows = slice(x * H, (x + 1) * H)
            work[k, x] = z_back(lines[rows, 0:N], lines[rows, N : 2 * N], zb, tall)
        return 0

    lax.fori_loop(0, 6, first_strain, 0)
    partial[...] = jnp.zeros_like(partial)

    def stress(chunk, _):
        rows = pl.ds(chunk * ROWS, ROWS)
        for x in range(2):
            parts = [work[i, x, rows, :] for i in range(6)]
            partial[0] += sum_squares(parts)
            xx, xy, xz, yy, yz, zz = parts
            value = polarize([xx, yy, zz, yz, xz, xy], conc[x, rows, :])
            for i, which in enumerate(ORDER):
                work[i, x, rows, :] = value[which]
        return 0

    lax.fori_loop(0, N // ROWS, stress, 0)

    def stress_ahead(k, _):
        for x in range(2):
            value = z_ahead(work[k, x], zf, tall)
            put_pair(wide, x, value[0:H], value[H:N])
        lines[...] = dot(wide[...], yf[...])

        @pl.when(k >= 3)
        def _():
            def mix(chunk, _):
                rows = pl.ds(chunk * ROWS, ROWS)
                index = chunk * ROWS + lax.broadcasted_iota(jnp.int32, (ROWS, N), 0)
                along_z = jnp.where(index < H, index, index - H).astype(F32) * STEP
                along_y = lane_wave(ROWS)
                for part in range(2):
                    lanes = slice(part * N, (part + 1) * N)
                    value = lines[rows, lanes]
                    lines[rows, lanes] = planes[rows, lanes] + along_z * value
                    planes[rows, lanes] = along_y * value
                return 0

            lax.fori_loop(0, N // ROWS, mix, 0)

        @pl.when(k != 3)
        def _():
            field = STRESS + jnp.where(k < 3, k, k - 1)
            store_planes(sent, field, lines)
            send(field)

        return 0

    planes[...] = jnp.zeros_like(planes)
    lax.fori_loop(0, 6, stress_ahead, 0)

    receive(CONC)
    plane_ahead(CONC, 0)
    conc_hat[...] = spectrum[0]
    along_y, along_z = lane_wave(N), me.astype(F32) * STEP

    def first_planes(k, _):
        for which, field, factor in (
            (XX, 0, None),
            (YY, 2, along_y * along_y),
            (ZZ, 2, along_z * along_z),
            (YZ, 2, along_y * along_z),
            (XZ, 1, along_z),
            (XY, 1, along_y),
        ):

            @pl.when(k == which)
            def _():
                plane_lines(kept.at[field], factor)

        before[k] = dot(wide[...], yb[...])
        return 0

    lax.fori_loop(0, 6, first_planes, 0)

    def stress_x(slot, _):
        receive(STRESS + slot)
        x_ahead(landed, STRESS + slot, xf, tall, spectrum, slot)
        return 0

    lax.fori_loop(0, 5, stress_x, 0)
    green_full(spectrum, me)

    real_weight = jnp.where(me == 0, 1.0, 2.0) * float(N)
    imag_weight = jnp.where(me == 0, 0.0, 2.0) * float(N)

    def shift_back(slot, _):
        plane_lines(x_lines(spectrum.at[slot], xb, tall))
        plane_back()
        scatter_cells(sent, SHIFT + slot, lines)
        send(SHIFT + slot)

        def squares(chunk, _):
            rows = pl.ds(chunk * ROWS, ROWS)
            real = lines[rows, 0:N] - before[slot, rows, 0:N]
            imag = lines[rows, N : 2 * N] - before[slot, rows, N : 2 * N]
            partial[1] += real_weight * (real * real) + imag_weight * (imag * imag)
            return 0

        lax.fori_loop(0, N // ROWS, squares, 0)
        return 0

    lax.fori_loop(0, 6, shift_back, 0)

    col_sums[col, 0:8, :] = fold(partial[0])
    col_sums[col, 8:16, :] = fold(partial[1])
    column_send(lambda t: col_sums.at[col], col_sums.at[col], 1)
    sums_src = col_sums.at[pl.ds(0, COLS - 1)]
    col_wait = side_copy(sums_src, sums_src, 1, (row, next_col))

    def strain_copy(k):
        return pltpu.make_async_copy(turned.at[k], strain_out.at[k], side_send.at[3 + k])

    def second_strain(k, _):
        receive(SHIFT + k)
        for half in range(2):
            work[k, half] = cells_back(SHIFT + k, half)
        return 0

    lax.fori_loop(0, 6, second_strain, 0)

    def drive(chunk, _):
        rows = pl.ds(chunk * ROWS, ROWS)
        for half in range(2):
            parts = [work[i, half, rows, :] for i in range(6)]
            planes[rows, half * N : (half + 1) * N] = potential(parts, cells[half, rows, :])
        return 0

    lax.fori_loop(0, N // ROWS, drive, 0)
    cells_ahead(DRIVE, lambda half: planes[:, half * N : (half + 1) * N])
    send(DRIVE)

    def strain_turn(k, _):
        for half in range(2):
            turned[k, 16 * half : 16 * half + 16] = work[k, half].T.reshape(16, 16, N)
        strain_copy(k).start()
        return 0

    lax.fori_loop(0, 6, strain_turn, 0)
    col_wait.wait_recv()
    total = col_sums[0]
    for i in range(1, COLS):
        total = total + col_sums[i]
    row_sums[row] = total

    def row_send(i, _):
        other = lax.rem(row + i, LINES)
        side_copy(row_sums.at[row], row_sums.at[row], 2, (other, col)).start()
        return 0

    lax.fori_loop(1, LINES, row_send, 0)
    rows_src = row_sums.at[pl.ds(0, LINES - 1)]
    row_wait = side_copy(rows_src, rows_src, 2, (lax.rem(row + 1, LINES), col))

    receive(DRIVE)
    plane_ahead(DRIVE, 0)
    relax(spectrum, 0, conc_hat, me)
    plane_lines(x_lines(spectrum.at[0], xb, tall))
    plane_back()
    scatter_cells(sent, NEXT, lines)
    send(NEXT)

    row_wait.wait_recv()
    total = row_sums[0]
    for i in range(1, LINES):
        total = total + row_sums[i]
    norms[...] = total
    row_wait.wait_send()
    col_wait.wait_send()
    plain_wait.wait_send()

    def sent_all(field, _):
        whole(field).wait_send()
        return 0

    lax.fori_loop(0, FIELDS, sent_all, 0)

    def strain_done(k, _):
        strain_copy(k).wait()
        return 0

    lax.fori_loop(0, 6, strain_done, 0)
    receive(NEXT)
    for half in range(2):
        result[16 * half : 16 * half + 16] = cells_back(NEXT, half).T.reshape(16, 16, N)


def shape(*dims):
    return jax.ShapeDtypeStruct(dims, F32)


def shards(base, concentration):
    vmem = pl.BlockSpec(memory_space=pltpu.VMEM)
    hbm = pl.BlockSpec(memory_space=pl.ANY)
    result, strain, norms = pl.pallas_call(
        step_kernel,
        out_shape=[shape(32, 16, N), shape(6, 32, 16, N), shape(16, H)],
        in_specs=[vmem, vmem],
        out_specs=[vmem, hbm, vmem],
        scratch_shapes=[
            pltpu.VMEM((FIELDS, 8 * H, H), F32),
            pltpu.VMEM((FIELDS, 8 * H, H), F32),
            pltpu.VMEM((2, N, N), F32),
            pltpu.VMEM((2, N, N), F32),
            pltpu.VMEM((2, N, N), F32),
            pltpu.VMEM((6, 2, N, N), F32),
            pltpu.VMEM((6, N, 2 * N), F32),
            pltpu.VMEM((3, 2 * N, N), F32),
            pltpu.VMEM((6, 32, 16, N), F32),
            pltpu.VMEM((6, 2 * N, N), F32),
            pltpu.VMEM((2 * N, N), F32),
            pltpu.VMEM((N, 2 * N), F32),
            pltpu.VMEM((N, 2 * N), F32),
            pltpu.VMEM((6 * N, N), B16),
            pltpu.VMEM((2 * H, 6 * N), B16),
            pltpu.VMEM((N, 3 * N), B16),
            pltpu.VMEM((N, 3 * N), B16),
            pltpu.VMEM((6 * N, 2 * N), B16),
            pltpu.VMEM((6 * N, 2 * N), B16),
            pltpu.VMEM((2 * N, 6 * N), B16),
            pltpu.VMEM((2 * N, 6 * N), B16),
            pltpu.VMEM((2, ROWS, N), F32),
            pltpu.VMEM((COLS, 16, H), F32),
            pltpu.VMEM((LINES, 16, H), F32),
            pltpu.SemaphoreType.DMA((FIELDS,)),
            pltpu.SemaphoreType.DMA((FIELDS,)),
            pltpu.SemaphoreType.DMA((9,)),
            pltpu.SemaphoreType.DMA((3,)),
        ],
        compiler_params=pltpu.CompilerParams(
            vmem_limit_bytes=60 * 2**20, has_side_effects=True
        ),
        name="step",
    )(base, concentration)
    sums = jnp.sum(norms.reshape(2, 8 * H), axis=1)
    return result, strain, jnp.sqrt(sums * SCALE)


def solution(mesh):
    base = base_tables()
    body = jax.shard_map(
        shards,
        mesh=mesh,
        in_specs=(P(), P("row", "col", None)),
        out_specs=(P("row", "col", None), P(None, "row", "col", None), P()),
        check_vma=False,
    )

    def run(concentration):
        return body(jnp.asarray(base), concentration)

    return run
```

```python
import math

import jax
import jax.numpy as jnp
import numpy as np
from jax import lax
from jax.experimental import pallas as pl
from jax.experimental.pallas import tpu as pltpu
from jax.sharding import PartitionSpec as P

F32 = jnp.float32
B16 = jnp.bfloat16
N = 256
H = 128
ITERS = 2
STEP = 2.0 * math.pi / N
SCALE = 1.0 / float(N) ** 3

FIRST_LOW = 1.0
FIRST_RISE = 0.6
SHEAR_LOW = 0.7
SHEAR_RISE = 0.8
FIRST_REF = 1.3
SHEAR_REF = 1.1
BETA_REF = 2.4 / 3.5
EIGEN_STRAIN = 0.5
WELL_HEIGHT = 1.0
TIME_STEP = 0.5
GRADIENT_ENERGY = 0.5

XX, YY, ZZ, YZ, XZ, XY = range(6)


def base_tables():
    index = np.arange(N)
    angle = (index[:, None] * index[None, :] % N) * (2.0 * np.pi / N)
    parts = []
    for table in (np.cos(angle), np.sin(angle)):
        lead = table.astype(np.float32).astype(jnp.bfloat16)
        rest = (table - lead.astype(np.float64)).astype(np.float32).astype(jnp.bfloat16)
        parts += [lead, rest]
    return np.stack(parts)


def split(value):
    lead = value.astype(B16)
    rest = (value - lead.astype(F32)).astype(B16)
    return lead, rest


def dot(a, b):
    return jnp.dot(a, b, preferred_element_type=F32)


def fill_left(base, out, sine_sign):
    for block, part in enumerate((0, 0, 1)):
        at = block * 2 * N
        cosine, sine = base[part], base[2 + part]
        upper, lower = (sine, -sine) if sine_sign > 0 else (-sine, sine)
        out[0:N, at : at + N] = cosine
        out[0:N, at + N : at + 2 * N] = upper
        out[N : 2 * N, at : at + N] = lower
        out[N : 2 * N, at + N : at + 2 * N] = cosine


def fill_right(base, out, sine_sign):
    for block, part in enumerate((0, 0, 1)):
        at = block * 2 * N
        cosine, sine = base[part], base[2 + part]
        upper, lower = (sine, -sine) if sine_sign > 0 else (-sine, sine)
        out[at : at + N, 0:N] = cosine
        out[at : at + N, N : 2 * N] = upper
        out[at + N : at + 2 * N, 0:N] = lower
        out[at + N : at + 2 * N, N : 2 * N] = cosine


def fill_z_ahead(base, out):
    for block, part in enumerate((0, 0, 1)):
        at = block * N
        out[0:H, at : at + N] = base[part, 0:H, :]
        out[H:N, at : at + N] = -base[2 + part, 0:H, :]


def fill_z_back(base, out):
    column = lax.broadcasted_iota(jnp.int32, (N, H), 1)
    weight = jnp.where(column == 0, 1.0, 2.0)
    for block, part in enumerate((0, 0, 1)):
        at = block * N
        out[:, at : at + H] = (base[part, :, 0:H].astype(F32) * weight).astype(B16)
        out[:, at + H : at + N] = (base[2 + part, :, 0:H].astype(F32) * -weight).astype(B16)


def put_pair(wide, x, real, imag):
    rows = pl.ds(x * H, H)
    for at, value in ((0, real), (N, imag)):
        lead, rest = split(value)
        wide[rows, at : at + N] = lead
        wide[rows, 2 * N + at : 3 * N + at] = rest
        wide[rows, 4 * N + at : 5 * N + at] = lead


def z_ahead(field, z_table, tall):
    lead, rest = split(field)
    tall[0:N, :] = lead
    tall[N : 2 * N, :] = rest
    tall[2 * N : 3 * N, :] = lead
    return dot(z_table[...], tall[0 : 3 * N, :])


def z_back(real, imag, z_table, tall):
    for at, value in ((0, real), (H, imag)):
        lead, rest = split(value)
        tall[at : at + H, :] = lead
        tall[N + at : N + at + H, :] = rest
        tall[2 * N + at : 2 * N + at + H, :] = lead
    return dot(z_table[...], tall[0 : 3 * N, :])


def store_planes(out, field, spectrum):
    for x in range(2):
        for block in range(4):
            out[field, pl.ds(x * 4 + block, H, stride=8), :] = spectrum[
                x * H : (x + 1) * H, block * H : (block + 1) * H
            ]


def load_plane(landed, field, x):
    parts = [landed[field, pl.ds(x * 4 + block, H, stride=8), :] for block in range(4)]
    return jnp.concatenate(parts[0:2], axis=1), jnp.concatenate(parts[2:4], axis=1)


def put_tall(tall, part, rows, lanes):
    lead, rest = split(rows)
    at = part * N
    tall[at : at + N, lanes] = lead
    tall[2 * N + at : 3 * N + at, lanes] = rest
    tall[4 * N + at : 5 * N + at, lanes] = lead


def x_ahead(landed, field, x_table, tall, spectrum, slot):
    for part in range(2):
        for half in range(2):
            rows = landed[field, pl.ds(part * 2 + half, N, stride=4), :]
            put_tall(tall, part, rows, slice(half * H, (half + 1) * H))
    spectrum[slot] = dot(x_table[...], tall[...])


def x_lines(source, x_table, tall):
    for part in range(2):
        put_tall(tall, part, source[part * N : (part + 1) * N], slice(0, N))
    return dot(x_table[...], tall[...])


def store_lines(out, field, lines):
    for part in range(2):
        for half in range(2):
            out[field, pl.ds(part * 2 + half, N, stride=4), :] = lines[
                part * N : (part + 1) * N, half * H : (half + 1) * H
            ]


def put_rows(wide, rows, at, value):
    lead, rest = split(value)
    count = value.shape[1]
    wide[rows, at : at + count] = lead
    wide[rows, 2 * N + at : 2 * N + at + count] = rest
    wide[rows, 4 * N + at : 4 * N + at + count] = lead


def turn_groups(value):
    row = lax.broadcasted_iota(jnp.int32, value.shape, 1)
    group = lax.broadcasted_iota(jnp.int32, value.shape, 2) // 16
    for bit in (1, 2, 4):
        row_set, group_set = (row & bit) != 0, (group & bit) != 0
        moved = pltpu.roll(pltpu.roll(value, 8 - bit, axis=1), 16 * bit, axis=2)
        if bit < 4:
            below = pltpu.roll(pltpu.roll(value, bit, axis=1), H - 16 * bit, axis=2)
            moved = jnp.where(group_set, moved, below)
        value = jnp.where(row_set == group_set, value, moved)
    return value


def tile_rows(block, part, high, which):
    return pl.ds(block * H + high * 64 + part * 4 + which, 8, stride=8)


def gather_cells(landed, field, wide):
    def go(block, _):
        for part in range(2):
            for high in range(2):
                parts = [landed[field, tile_rows(block, part, high, i), :] for i in range(4)]
                value = turn_groups(jnp.stack(parts)).reshape(32, H)
                put_rows(wide, pl.ds(block * 32, 32), part * N + high * H, value)
        return 0

    lax.fori_loop(0, 8, go, 0)


def scatter_block(out, field, lines, block):
    for part in range(2):
        for high in range(2):
            at = part * N + high * H
            value = lines[pl.ds(pl.multiple_of(block * 32, 32), 32), at : at + H]
            value = turn_groups(value.reshape(4, 8, H))
            for i in range(4):
                out[field, tile_rows(block, part, high, i), :] = value[i]


def signed(index):
    return jnp.where(index < H, index, index - N).astype(F32) * STEP


def lane_wave(rows, lanes=N):
    return signed(lax.broadcasted_iota(jnp.int32, (rows, lanes), 1))


def row_wave_z():
    return lax.broadcasted_iota(jnp.int32, (H, N), 0).astype(F32) * STEP


CHUNK = 32


def chunk_waves(chunk, kz):
    row = chunk * CHUNK + lax.broadcasted_iota(jnp.int32, (CHUNK, N), 0)
    wave_x = signed(row)
    wave_y = lane_wave(CHUNK)
    wave_z = kz.astype(F32) * STEP
    square = wave_x * wave_x + wave_y * wave_y + wave_z * wave_z
    return wave_x, wave_y, wave_z, square


def green_first(spectrum, source, kz):
    def body(chunk, _):
        wave_x, wave_y, wave_z, square = chunk_waves(chunk, kz)
        nonzero = square > 0.0
        safe = jnp.where(nonzero, square, 1.0)
        factor = jnp.where(nonzero, (BETA_REF - 1.0) * SCALE / (SHEAR_REF * safe), 0.0)
        for part in range(2):
            rows = pl.ds(part * N + chunk * CHUNK, CHUNK)
            psi = spectrum[source, rows, :] * factor
            once = wave_x * psi
            spectrum[0, rows, :] = wave_x * once
            spectrum[1, rows, :] = once
            spectrum[2, rows, :] = psi
        return 0

    lax.fori_loop(0, N // CHUNK, body, 0)


def green_full(spectrum, kz):
    def body(chunk, _):
        wave_x, wave_y, wave_z, square = chunk_waves(chunk, kz)
        nonzero = square > 0.0
        safe = jnp.where(nonzero, square, 1.0)
        scale = jnp.where(nonzero, -SCALE / (SHEAR_REF * safe), 0.0)
        ratio = BETA_REF / safe
        for part in range(2):
            rows = pl.ds(part * N + chunk * CHUNK, CHUNK)
            first, second, third = (spectrum[slot, rows, :] for slot in range(3))
            force_x = wave_x * first + wave_y * second + wave_z * third
            force_y = wave_x * second + spectrum[3, rows, :]
            force_z = wave_x * third + spectrum[4, rows, :]
            along = (wave_x * force_x + wave_y * force_y + wave_z * force_z) * ratio
            moved_x = scale * (force_x - along * wave_x)
            moved_y = scale * (force_y - along * wave_y)
            moved_z = scale * (force_z - along * wave_z)
            spectrum[XX, rows, :] = wave_x * moved_x
            spectrum[YY, rows, :] = wave_y * moved_y
            spectrum[ZZ, rows, :] = wave_z * moved_z
            spectrum[YZ, rows, :] = 0.5 * (wave_y * moved_z + wave_z * moved_y)
            spectrum[XZ, rows, :] = 0.5 * (wave_x * moved_z + wave_z * moved_x)
            spectrum[XY, rows, :] = 0.5 * (wave_x * moved_y + wave_y * moved_x)
        return 0

    lax.fori_loop(0, N // CHUNK, body, 0)


def relax(spectrum, drive, conc, kz):
    def body(chunk, _):
        _, _, _, square = chunk_waves(chunk, kz)
        inverse = SCALE / (1.0 + TIME_STEP * GRADIENT_ENERGY * square * square)
        for part in range(2):
            rows = pl.ds(part * N + chunk * CHUNK, CHUNK)
            value = conc[rows, :] - TIME_STEP * square * spectrum[drive, rows, :]
            spectrum[drive, rows, :] = value * inverse
        return 0

    lax.fori_loop(0, N // CHUNK, body, 0)


ROWS = 32


def eigen_stress(conc):
    rise = (3.0 * FIRST_RISE + 2.0 * SHEAR_RISE) * EIGEN_STRAIN
    low = (3.0 * FIRST_LOW + 2.0 * SHEAR_LOW) * EIGEN_STRAIN
    return (0.5 - conc) * (rise * (conc + 0.5) + low)


def polarize(parts, conc):
    first = FIRST_LOW + FIRST_RISE * conc
    excess = 2.0 * (SHEAR_LOW + SHEAR_RISE * conc - SHEAR_REF)
    normal = (first - FIRST_REF) * (parts[0] + parts[1] + parts[2]) + eigen_stress(conc)
    return [normal + excess * p for p in parts[:3]] + [excess * p for p in parts[3:]]


def potential(parts, conc):
    first = FIRST_LOW + FIRST_RISE * conc
    shear = SHEAR_LOW + SHEAR_RISE * conc
    dilation = EIGEN_STRAIN * conc
    d = [p - dilation for p in parts[:3]]
    trace = d[0] + d[1] + d[2]
    energy = d[0] * d[0] + d[1] * d[1] + d[2] * d[2]
    energy = energy + 2.0 * (parts[3] * parts[3] + parts[4] * parts[4] + parts[5] * parts[5])
    chemical = 2.0 * WELL_HEIGHT * conc * (1.0 - conc) * (1.0 - 2.0 * conc)
    return (
        chemical
        + 0.5 * FIRST_RISE * trace * trace
        + SHEAR_RISE * energy
        - EIGEN_STRAIN * (3.0 * first + 2.0 * shear) * trace
    )


def sum_squares(parts):
    total = parts[0] * parts[0]
    for part in parts[1:]:
        total = total + part * part
    return total


def fold(value):
    tile = value[0:8, 0:H] + value[0:8, H:N]
    for at in range(8, ROWS, 8):
        tile = tile + (value[at : at + 8, 0:H] + value[at : at + 8, H:N])
    return tile


ORDER = (YY, YZ, ZZ, XY, XZ, XX)
PRESSURE, CONC, FIRST, STRESS, SHIFT, DRIVE, NEXT = 0, 1, 2, 5, 10, 16, 17
FIELDS = 18
COLS, LINES = 16, 8
MESH = pl.DeviceIdType.MESH


def step_kernel(
    base_hbm,
    concentration_hbm,
    result,
    strain_out,
    norms,
    base,
    concentration,
    landed,
    sent,
    plain,
    cells,
    conc,
    work,
    before,
    kept,
    turned,
    spectrum,
    conc_hat,
    planes,
    lines,
    tall,
    wide,
    zf,
    zb,
    yf,
    yb,
    xf,
    xb,
    partial,
    col_sums,
    row_sums,
    send_sems,
    recv_sems,
    side_send,
    side_recv,
):
    row, col = lax.axis_index("row"), lax.axis_index("col")
    me = row * COLS + col
    next_col = lax.rem(col + 1, COLS)

    def tiles(ref, field, device):
        return ref.at[field, pl.ds(pl.multiple_of(device * 8, 8), 8), :]

    def row_at(step):
        return lax.rem(row + step, LINES)

    def each_device(step, act):
        for shift in range(1 if isinstance(step, int) and step == 0 else 0, COLS):
            act(row_at(step), lax.rem(col + shift, COLS))

    def send_row(field, step):
        def go(other_row, other_col):
            other = other_row * COLS + other_col
            pltpu.make_async_remote_copy(
                src_ref=tiles(sent, field, other),
                dst_ref=tiles(landed, field, me),
                send_sem=send_sems.at[field],
                recv_sem=recv_sems.at[field],
                device_id=(other_row, other_col),
                device_id_type=MESH,
            ).start()

        each_device(step, go)

    def keep_own(field):
        own = pl.ds(pl.multiple_of(me * 8, 8), 8)
        landed[field, own, :] = sent[field, own, :]

    def send(field):
        send_row(field, 0)

        def go(step, _):
            send_row(field, step)
            return 0

        lax.fori_loop(1, LINES, go, 0)
        keep_own(field)

    def scatter_send(field):
        scatter_block(sent, field, lines, row)
        send_row(field, 0)
        scatter_block(sent, field, lines, row_at(1))

        def go(step, _):
            send_row(field, step)
            scatter_block(sent, field, lines, row_at(step + 1))
            return 0

        lax.fori_loop(1, LINES - 1, go, 0)
        send_row(field, LINES - 1)
        keep_own(field)

    def whole(field):
        rows = pl.ds(0, 127 * 8)
        return pltpu.make_async_remote_copy(
            src_ref=sent.at[field, rows, :],
            dst_ref=landed.at[field, rows, :],
            send_sem=send_sems.at[field],
            recv_sem=recv_sems.at[field],
            device_id=(row, next_col),
            device_id_type=MESH,
        )

    def receive(field):
        whole(field).wait_recv()

    def side_copy(src, dst, index, device):
        return pltpu.make_async_remote_copy(
            src_ref=src,
            dst_ref=dst,
            send_sem=side_send.at[index],
            recv_sem=side_recv.at[index],
            device_id=device,
            device_id_type=MESH,
        )

    def column_send(src_of, dst, index):
        def go(i, _):
            target = lax.rem(col + i, COLS)
            side_copy(src_of(target), dst, index, (row, target)).start()
            return 0

        lax.fori_loop(1, COLS, go, 0)

    def lines_of(device):
        return pl.ds(pl.multiple_of(device * 16, 16), 16)

    def pair_of(device):
        return pl.ds(device * 2, 2)


    def cells_ahead(field, field_of):
        for half in range(2):
            value = z_ahead(field_of(half), zf, tall)
            for part in range(2):
                for j in range(2):
                    sent[field, pl.ds(part * 4 + 2 * half + j, H, stride=8), :] = value[
                        part * H : (part + 1) * H, j * H : (j + 1) * H
                    ]

    def cells_back(field, half):
        parts = [landed[field, pl.ds(i, H, stride=8), :] for i in range(8)]
        real = jnp.concatenate(parts[2 * half : 2 * half + 2], axis=1)
        imag = jnp.concatenate(parts[4 + 2 * half : 6 + 2 * half], axis=1)
        return z_back(real, imag, zb, tall)

    def plane_ahead(field, slot):
        gather_cells(landed, field, wide)
        lines[...] = dot(wide[...], yf[...])
        for part in range(2):
            put_tall(tall, part, lines[:, part * N : (part + 1) * N], slice(0, N))
        spectrum[slot] = dot(xf[...], tall[...])

    def plane_lines(value, factor=None):
        for part in range(2):
            rows = value[part * N : (part + 1) * N]
            if factor is not None:
                rows = factor * rows
            put_rows(wide, slice(0, N), part * N, rows)

    def plane_back():
        lines[...] = dot(wide[...], yb[...])

    concentration_in = pltpu.make_async_copy(concentration_hbm, concentration, side_send.at[10])
    concentration_in.start()
    base_in = pltpu.make_async_copy(base_hbm, base, side_send.at[11])
    base_in.start()
    barrier = pltpu.get_barrier_semaphore()

    def greet(other_row, other_col):
        pl.semaphore_signal(
            barrier, inc=1, device_id=(other_row, other_col), device_id_type=MESH
        )

    each_device(0, greet)

    def greet_row(step, _):
        each_device(step, greet)
        return 0

    lax.fori_loop(1, LINES, greet_row, 0)
    concentration_in.wait()
    base_in.wait()
    fill_z_ahead(base, zf)
    for half in range(2):
        block = concentration[16 * half : 16 * half + 16].reshape(N, N)
        cells[half] = block.T

    def first_pressure(half):
        return eigen_stress(cells[half])

    cells_ahead(PRESSURE, first_pressure)
    fill_right(base, yf, -1)
    fill_left(base, xf, 1)
    fill_left(base, xb, -1)
    pl.semaphore_wait(barrier, 127)
    send(PRESSURE)
    fill_z_back(base, zb)
    fill_right(base, yb, 1)
    cells_ahead(CONC, lambda half: cells[half])

    receive(PRESSURE)
    column_send(lambda t: concentration.at[pair_of(t)], plain.at[:, lines_of(col), :], 0)
    plain[:, lines_of(col), :] = concentration[pair_of(col)]
    plain_src, plain_dst = concentration.at[pl.ds(0, 30)], plain.at[:, pl.ds(0, 240), :]
    plain_wait = side_copy(plain_src, plain_dst, 0, (row, next_col))
    plane_ahead(PRESSURE, 3)
    green_first(spectrum, 3, me)

    def first_back(step, _):
        slot = 2 - step
        kept[slot] = x_lines(spectrum.at[slot], xb, tall)
        store_lines(sent, FIRST + slot, kept.at[slot])
        send(FIRST + slot)
        return 0

    lax.fori_loop(0, 3, first_back, 0)
    plain_wait.wait_recv()
    for x in range(2):
        conc[x] = plain[x].T

    wave_y, wave_z = lane_wave(H), row_wave_z()

    def first_strain(k, _):
        for slot, field, factor in (
            (0, 2, wave_y * wave_y),
            (1, 2, wave_y * wave_z),
            (2, 2, wave_z * wave_z),
            (3, 1, wave_y),
            (4, 1, wave_z),
            (5, 0, None),
        ):

            @pl.when(k == slot)
            def _():
                if slot in (0, 3, 5):
                    receive(FIRST + field)
                for x in range(2):
                    real, imag = load_plane(landed, FIRST + field, x)
                    if factor is not None:
                        real, imag = factor * real, factor * imag
                    put_pair(wide, x, real, imag)

        plane_back()
        for x in range(2):
            rows = slice(x * H, (x + 1) * H)
            work[k, x] = z_back(lines[rows, 0:N], lines[rows, N : 2 * N], zb, tall)
        return 0

    lax.fori_loop(0, 6, first_strain, 0)
    partial[...] = jnp.zeros_like(partial)

    def stress(chunk, _):
        rows = pl.ds(chunk * ROWS, ROWS)
        for x in range(2):
            parts = [work[i, x, rows, :] for i in range(6)]
            partial[0] += sum_squares(parts)
            yy, yz, zz, xy, xz, xx = parts
            value = polarize([xx, yy, zz, yz, xz, xy], conc[x, rows, :])
            for i, which in enumerate(ORDER):
                work[i, x, rows, :] = value[which]
        return 0

    lax.fori_loop(0, N // ROWS, stress, 0)

    def stress_ahead(k, _):
        slot = jnp.where(k == 0, 5, jnp.where(k < 3, k + 2, k - 3))
        for x in range(2):
            value = z_ahead(work[slot, x], zf, tall)
            put_pair(wide, x, value[0:H], value[H:N])
        lines[...] = dot(wide[...], yf[...])

        @pl.when(k >= 3)
        def _():
            def mix(chunk, _):
                rows = pl.ds(chunk * ROWS, ROWS)
                index = chunk * ROWS + lax.broadcasted_iota(jnp.int32, (ROWS, N), 0)
                along_z = jnp.where(index < H, index, index - H).astype(F32) * STEP
                along_y = lane_wave(ROWS)
                for part in range(2):
                    lanes = slice(part * N, (part + 1) * N)
                    value = lines[rows, lanes]
                    lines[rows, lanes] = planes[rows, lanes] + along_z * value
                    planes[rows, lanes] = along_y * value
                return 0

            lax.fori_loop(0, N // ROWS, mix, 0)

        @pl.when(k != 3)
        def _():
            field = STRESS + jnp.where(k < 3, k, k - 1)
            store_planes(sent, field, lines)
            send(field)

        return 0

    planes[...] = jnp.zeros_like(planes)
    lax.fori_loop(0, 6, stress_ahead, 0)

    along_y, along_z = lane_wave(N), me.astype(F32) * STEP

    def first_planes(k, _):
        for which, field, factor in (
            (XX, 0, None),
            (YY, 2, along_y * along_y),
            (ZZ, 2, along_z * along_z),
            (YZ, 2, along_y * along_z),
            (XZ, 1, along_z),
            (XY, 1, along_y),
        ):

            @pl.when(k == which)
            def _():
                plane_lines(kept.at[field], factor)

        before[k] = dot(wide[...], yb[...])
        return 0

    lax.fori_loop(0, 6, first_planes, 0)

    def stress_x(slot, _):
        receive(STRESS + slot)
        x_ahead(landed, STRESS + slot, xf, tall, spectrum, slot)
        return 0

    lax.fori_loop(0, 5, stress_x, 0)
    green_full(spectrum, me)

    real_weight = jnp.where(me == 0, 1.0, 2.0) * float(N)
    imag_weight = jnp.where(me == 0, 0.0, 2.0) * float(N)

    def shift_back(slot, _):
        plane_lines(x_lines(spectrum.at[slot], xb, tall))
        plane_back()
        scatter_send(SHIFT + slot)

        def squares(chunk, _):
            rows = pl.ds(chunk * ROWS, ROWS)
            real = lines[rows, 0:N] - before[slot, rows, 0:N]
            imag = lines[rows, N : 2 * N] - before[slot, rows, N : 2 * N]
            partial[1] += real_weight * (real * real) + imag_weight * (imag * imag)
            return 0

        lax.fori_loop(0, N // ROWS, squares, 0)
        return 0

    lax.fori_loop(0, 6, shift_back, 0)
    send(CONC)

    col_sums[col, 0:8, :] = fold(partial[0])
    col_sums[col, 8:16, :] = fold(partial[1])
    column_send(lambda t: col_sums.at[col], col_sums.at[col], 1)
    sums_src = col_sums.at[pl.ds(0, COLS - 1)]
    col_wait = side_copy(sums_src, sums_src, 1, (row, next_col))

    def strain_copy(k):
        return pltpu.make_async_copy(turned.at[k], strain_out.at[k], side_send.at[3 + k])

    def second_strain(k, _):
        receive(SHIFT + k)
        for half in range(2):
            work[k, half] = cells_back(SHIFT + k, half)
        return 0

    lax.fori_loop(0, 6, second_strain, 0)

    def drive(chunk, _):
        rows = pl.ds(chunk * ROWS, ROWS)
        for half in range(2):
            parts = [work[i, half, rows, :] for i in range(6)]
            planes[rows, half * N : (half + 1) * N] = potential(parts, cells[half, rows, :])
        return 0

    lax.fori_loop(0, N // ROWS, drive, 0)
    cells_ahead(DRIVE, lambda half: planes[:, half * N : (half + 1) * N])
    send(DRIVE)

    def strain_turn(k, _):
        for half in range(2):
            turned[k, 16 * half : 16 * half + 16] = 2.0 * work[k, half].T.reshape(16, 16, N)
        strain_copy(k).start()
        return 0

    lax.fori_loop(0, 6, strain_turn, 0)
    receive(CONC)
    plane_ahead(CONC, 0)
    conc_hat[...] = spectrum[0]
    col_wait.wait_recv()
    total = col_sums[0]
    for i in range(1, COLS):
        total = total + col_sums[i]
    row_sums[row] = total

    def row_send(i, _):
        other = lax.rem(row + i, LINES)
        side_copy(row_sums.at[row], row_sums.at[row], 2, (other, col)).start()
        return 0

    lax.fori_loop(1, LINES, row_send, 0)
    rows_src = row_sums.at[pl.ds(0, LINES - 1)]
    row_wait = side_copy(rows_src, rows_src, 2, (lax.rem(row + 1, LINES), col))

    receive(DRIVE)
    plane_ahead(DRIVE, 0)
    relax(spectrum, 0, conc_hat, me)
    plane_lines(x_lines(spectrum.at[0], xb, tall))
    plane_back()
    scatter_send(NEXT)

    row_wait.wait_recv()
    total = row_sums[0]
    for i in range(1, LINES):
        total = total + row_sums[i]
    norms[...] = total
    row_wait.wait_send()
    col_wait.wait_send()
    plain_wait.wait_send()

    def sent_all(field, _):
        whole(field).wait_send()
        return 0

    lax.fori_loop(0, FIELDS, sent_all, 0)

    def strain_done(k, _):
        strain_copy(k).wait()
        return 0

    lax.fori_loop(0, 6, strain_done, 0)
    receive(NEXT)
    copies = []
    for half in range(2):
        planes_x = pl.ds(16 * half, 16)
        turned[0, planes_x] = 2.0 * cells_back(NEXT, half).T.reshape(16, 16, N)
        copies.append(
            pltpu.make_async_copy(
                turned.at[0, planes_x], result.at[planes_x], side_send.at[9 + half]
            )
        )
        copies[-1].start()
    for copy in copies:
        copy.wait()


def shape(*dims):
    return jax.ShapeDtypeStruct(dims, F32)


def shards(base, concentration):
    vmem = pl.BlockSpec(memory_space=pltpu.VMEM)
    hbm = pl.BlockSpec(memory_space=pl.ANY)
    hbm_in = pl.BlockSpec(memory_space=pltpu.HBM)
    result, strain, norms = pl.pallas_call(
        step_kernel,
        out_shape=[shape(32, 16, N), shape(6, 32, 16, N), shape(16, H)],
        in_specs=[hbm_in, hbm_in],
        out_specs=[hbm, hbm, vmem],
        scratch_shapes=[
            pltpu.VMEM((4, N, N), B16),
            pltpu.VMEM((32, 16, N), F32),
            pltpu.VMEM((FIELDS, 8 * H, H), F32),
            pltpu.VMEM((FIELDS, 8 * H, H), F32),
            pltpu.VMEM((2, N, N), F32),
            pltpu.VMEM((2, N, N), F32),
            pltpu.VMEM((2, N, N), F32),
            pltpu.VMEM((6, 2, N, N), F32),
            pltpu.VMEM((6, N, 2 * N), F32),
            pltpu.VMEM((3, 2 * N, N), F32),
            pltpu.VMEM((6, 32, 16, N), F32),
            pltpu.VMEM((6, 2 * N, N), F32),
            pltpu.VMEM((2 * N, N), F32),
            pltpu.VMEM((N, 2 * N), F32),
            pltpu.VMEM((N, 2 * N), F32),
            pltpu.VMEM((6 * N, N), B16),
            pltpu.VMEM((2 * H, 6 * N), B16),
            pltpu.VMEM((N, 3 * N), B16),
            pltpu.VMEM((N, 3 * N), B16),
            pltpu.VMEM((6 * N, 2 * N), B16),
            pltpu.VMEM((6 * N, 2 * N), B16),
            pltpu.VMEM((2 * N, 6 * N), B16),
            pltpu.VMEM((2 * N, 6 * N), B16),
            pltpu.VMEM((2, ROWS, N), F32),
            pltpu.VMEM((COLS, 16, H), F32),
            pltpu.VMEM((LINES, 16, H), F32),
            pltpu.SemaphoreType.DMA((FIELDS,)),
            pltpu.SemaphoreType.DMA((FIELDS,)),
            pltpu.SemaphoreType.DMA((12,)),
            pltpu.SemaphoreType.DMA((3,)),
        ],
        compiler_params=pltpu.CompilerParams(
            vmem_limit_bytes=48 * 2**20, has_side_effects=True, collective_id=0
        ),
        name="step",
    )(base, concentration)
    sums = jnp.sum(norms.reshape(2, 8 * H), axis=1)
    return 0.5 * result, 0.5 * strain, jnp.sqrt(sums * SCALE)


def solution(mesh):
    base = base_tables()
    body = jax.shard_map(
        shards,
        mesh=mesh,
        in_specs=(P(), P("row", "col", None)),
        out_specs=(P("row", "col", None), P(None, "row", "col", None), P()),
        check_vma=False,
    )

    def run(concentration):
        return body(jnp.asarray(base), concentration)

    return run
```

```python
import math

import jax
import jax.numpy as jnp
import numpy as np
from jax import lax
from jax.experimental import pallas as pl
from jax.experimental.pallas import tpu as pltpu
from jax.sharding import PartitionSpec as P

F32 = jnp.float32
B16 = jnp.bfloat16
N = 256
H = 128
ITERS = 2
STEP = 2.0 * math.pi / N
SCALE = 1.0 / float(N) ** 3

FIRST_LOW = 1.0
FIRST_RISE = 0.6
SHEAR_LOW = 0.7
SHEAR_RISE = 0.8
FIRST_REF = 1.3
SHEAR_REF = 1.1
BETA_REF = 2.4 / 3.5
EIGEN_STRAIN = 0.5
WELL_HEIGHT = 1.0
TIME_STEP = 0.5
GRADIENT_ENERGY = 0.5

XX, YY, ZZ, YZ, XZ, XY = range(6)


def base_tables():
    index = np.arange(N)
    angle = (index[:, None] * index[None, :] % N) * (2.0 * np.pi / N)
    parts = []
    for table in (np.cos(angle), np.sin(angle)):
        lead = table.astype(np.float32).astype(jnp.bfloat16)
        rest = (table - lead.astype(np.float64)).astype(np.float32).astype(jnp.bfloat16)
        parts += [lead, rest]
    return np.stack(parts)


def split(value):
    lead = value.astype(B16)
    rest = (value - lead.astype(F32)).astype(B16)
    return lead, rest


def dot(a, b):
    return jnp.dot(a, b, preferred_element_type=F32)


def fill_left(base, out, sine_sign):
    for block, part in enumerate((0, 0, 1)):
        at = block * 2 * N
        cosine, sine = base[part], base[2 + part]
        upper, lower = (sine, -sine) if sine_sign > 0 else (-sine, sine)
        out[0:N, at : at + N] = cosine
        out[0:N, at + N : at + 2 * N] = upper
        out[N : 2 * N, at : at + N] = lower
        out[N : 2 * N, at + N : at + 2 * N] = cosine


def fill_right(base, out, sine_sign):
    for block, part in enumerate((0, 0, 1)):
        at = block * 2 * N
        cosine, sine = base[part], base[2 + part]
        upper, lower = (sine, -sine) if sine_sign > 0 else (-sine, sine)
        out[at : at + N, 0:N] = cosine
        out[at : at + N, N : 2 * N] = upper
        out[at + N : at + 2 * N, 0:N] = lower
        out[at + N : at + 2 * N, N : 2 * N] = cosine


def fill_z_ahead(base, out):
    for block, part in enumerate((0, 0, 1)):
        at = block * N
        out[0:H, at : at + N] = base[part, 0:H, :]
        out[H:N, at : at + N] = -base[2 + part, 0:H, :]


def fill_z_back(base, out):
    column = lax.broadcasted_iota(jnp.int32, (N, H), 1)
    weight = jnp.where(column == 0, 1.0, 2.0)
    for block, part in enumerate((0, 0, 1)):
        at = block * N
        out[:, at : at + H] = (base[part, :, 0:H].astype(F32) * weight).astype(B16)
        out[:, at + H : at + N] = (base[2 + part, :, 0:H].astype(F32) * -weight).astype(B16)


def put_pair(wide, x, real, imag):
    rows = pl.ds(x * H, H)
    for at, value in ((0, real), (N, imag)):
        lead, rest = split(value)
        wide[rows, at : at + N] = lead
        wide[rows, 2 * N + at : 3 * N + at] = rest
        wide[rows, 4 * N + at : 5 * N + at] = lead


def z_ahead(field, z_table, tall):
    lead, rest = split(field)
    tall[0:N, :] = lead
    tall[N : 2 * N, :] = rest
    tall[2 * N : 3 * N, :] = lead
    return dot(z_table[...], tall[0 : 3 * N, :])


def z_back(real, imag, z_table, tall):
    for at, value in ((0, real), (H, imag)):
        lead, rest = split(value)
        tall[at : at + H, :] = lead
        tall[N + at : N + at + H, :] = rest
        tall[2 * N + at : 2 * N + at + H, :] = lead
    return dot(z_table[...], tall[0 : 3 * N, :])


def store_planes(out, field, spectrum):
    for x in range(2):
        for block in range(4):
            out[field, pl.ds(x * 4 + block, H, stride=8), :] = spectrum[
                x * H : (x + 1) * H, block * H : (block + 1) * H
            ]


def load_plane(landed, field, x):
    parts = [landed[field, pl.ds(x * 4 + block, H, stride=8), :] for block in range(4)]
    return jnp.concatenate(parts[0:2], axis=1), jnp.concatenate(parts[2:4], axis=1)


def put_tall(tall, part, rows, lanes):
    lead, rest = split(rows)
    at = part * N
    tall[at : at + N, lanes] = lead
    tall[2 * N + at : 3 * N + at, lanes] = rest
    tall[4 * N + at : 5 * N + at, lanes] = lead


def x_ahead(landed, field, x_table, tall, spectrum, slot):
    for part in range(2):
        for half in range(2):
            rows = landed[field, pl.ds(part * 2 + half, N, stride=4), :]
            put_tall(tall, part, rows, slice(half * H, (half + 1) * H))
    spectrum[slot] = dot(x_table[...], tall[...])


def x_lines(source, x_table, tall):
    for part in range(2):
        put_tall(tall, part, source[part * N : (part + 1) * N], slice(0, N))
    return dot(x_table[...], tall[...])


def store_lines(out, field, lines):
    for part in range(2):
        for half in range(2):
            out[field, pl.ds(part * 2 + half, N, stride=4), :] = lines[
                part * N : (part + 1) * N, half * H : (half + 1) * H
            ]


def put_rows(wide, rows, at, value):
    lead, rest = split(value)
    count = value.shape[1]
    wide[rows, at : at + count] = lead
    wide[rows, 2 * N + at : 2 * N + at + count] = rest
    wide[rows, 4 * N + at : 4 * N + at + count] = lead


def turn_groups(value):
    row = lax.broadcasted_iota(jnp.int32, value.shape, 1)
    group = lax.broadcasted_iota(jnp.int32, value.shape, 2) // 16
    for bit in (1, 2, 4):
        row_set, group_set = (row & bit) != 0, (group & bit) != 0
        moved = pltpu.roll(pltpu.roll(value, 8 - bit, axis=1), 16 * bit, axis=2)
        if bit < 4:
            below = pltpu.roll(pltpu.roll(value, bit, axis=1), H - 16 * bit, axis=2)
            moved = jnp.where(group_set, moved, below)
        value = jnp.where(row_set == group_set, value, moved)
    return value


def tile_rows(block, part, high, which):
    return pl.ds(block * H + high * 64 + part * 4 + which, 8, stride=8)


def gather_cells(landed, field, wide):
    def go(block, _):
        where = [(part, high) for part in range(2) for high in range(2)]
        tiles = [
            landed[field, tile_rows(block, part, high, i), :]
            for part, high in where
            for i in range(4)
        ]
        value = turn_groups(jnp.stack(tiles)).reshape(4, 32, H)
        for at, (part, high) in enumerate(where):
            put_rows(wide, pl.ds(block * 32, 32), part * N + high * H, value[at])
        return 0

    lax.fori_loop(0, 8, go, 0, unroll=2)


def scatter_block(out, field, lines, block):
    rows = pl.ds(pl.multiple_of(block * 32, 32), 32)
    groups = [lines[rows, at * H : (at + 1) * H].reshape(4, 8, H) for at in range(4)]
    value = turn_groups(jnp.concatenate(groups, axis=0))
    for at in range(4):
        for i in range(4):
            out[field, tile_rows(block, at // 2, at % 2, i), :] = value[at * 4 + i]


def signed(index):
    return jnp.where(index < H, index, index - N).astype(F32) * STEP


def lane_wave(rows, lanes=N):
    return signed(lax.broadcasted_iota(jnp.int32, (rows, lanes), 1))


def row_wave_z():
    return lax.broadcasted_iota(jnp.int32, (H, N), 0).astype(F32) * STEP


CHUNK = 32


def chunk_waves(chunk, kz):
    row = chunk * CHUNK + lax.broadcasted_iota(jnp.int32, (CHUNK, N), 0)
    wave_x = signed(row)
    wave_y = lane_wave(CHUNK)
    wave_z = kz.astype(F32) * STEP
    square = wave_x * wave_x + wave_y * wave_y + wave_z * wave_z
    return wave_x, wave_y, wave_z, square


def green_first(spectrum, source, kz):
    def body(chunk, _):
        wave_x, wave_y, wave_z, square = chunk_waves(chunk, kz)
        nonzero = square > 0.0
        safe = jnp.where(nonzero, square, 1.0)
        factor = jnp.where(nonzero, (BETA_REF - 1.0) * SCALE / (SHEAR_REF * safe), 0.0)
        for part in range(2):
            rows = pl.ds(part * N + chunk * CHUNK, CHUNK)
            psi = spectrum[source, rows, :] * factor
            once = wave_x * psi
            spectrum[0, rows, :] = wave_x * once
            spectrum[1, rows, :] = once
            spectrum[2, rows, :] = psi
        return 0

    lax.fori_loop(0, N // CHUNK, body, 0)


def green_full(spectrum, kz):
    def body(chunk, _):
        wave_x, wave_y, wave_z, square = chunk_waves(chunk, kz)
        nonzero = square > 0.0
        safe = jnp.where(nonzero, square, 1.0)
        scale = jnp.where(nonzero, -SCALE / (SHEAR_REF * safe), 0.0)
        ratio = BETA_REF / safe
        for part in range(2):
            rows = pl.ds(part * N + chunk * CHUNK, CHUNK)
            first, second, third = (spectrum[slot, rows, :] for slot in range(3))
            force_x = wave_x * first + wave_y * second + wave_z * third
            force_y = wave_x * second + spectrum[3, rows, :]
            force_z = wave_x * third + spectrum[4, rows, :]
            along = (wave_x * force_x + wave_y * force_y + wave_z * force_z) * ratio
            moved_x = scale * (force_x - along * wave_x)
            moved_y = scale * (force_y - along * wave_y)
            moved_z = scale * (force_z - along * wave_z)
            spectrum[XX, rows, :] = wave_x * moved_x
            spectrum[YY, rows, :] = wave_y * moved_y
            spectrum[ZZ, rows, :] = wave_z * moved_z
            spectrum[YZ, rows, :] = 0.5 * (wave_y * moved_z + wave_z * moved_y)
            spectrum[XZ, rows, :] = 0.5 * (wave_x * moved_z + wave_z * moved_x)
            spectrum[XY, rows, :] = 0.5 * (wave_x * moved_y + wave_y * moved_x)
        return 0

    lax.fori_loop(0, N // CHUNK, body, 0)


def relax(spectrum, drive, conc, kz):
    def body(chunk, _):
        _, _, _, square = chunk_waves(chunk, kz)
        inverse = SCALE / (1.0 + TIME_STEP * GRADIENT_ENERGY * square * square)
        for part in range(2):
            rows = pl.ds(part * N + chunk * CHUNK, CHUNK)
            value = conc[rows, :] - TIME_STEP * square * spectrum[drive, rows, :]
            spectrum[drive, rows, :] = value * inverse
        return 0

    lax.fori_loop(0, N // CHUNK, body, 0)


ROWS = 32


def eigen_stress(conc):
    rise = (3.0 * FIRST_RISE + 2.0 * SHEAR_RISE) * EIGEN_STRAIN
    low = (3.0 * FIRST_LOW + 2.0 * SHEAR_LOW) * EIGEN_STRAIN
    return (0.5 - conc) * (rise * (conc + 0.5) + low)


def polarize(parts, conc):
    first = FIRST_LOW + FIRST_RISE * conc
    excess = 2.0 * (SHEAR_LOW + SHEAR_RISE * conc - SHEAR_REF)
    normal = (first - FIRST_REF) * (parts[0] + parts[1] + parts[2]) + eigen_stress(conc)
    return [normal + excess * p for p in parts[:3]] + [excess * p for p in parts[3:]]


def potential(parts, conc):
    first = FIRST_LOW + FIRST_RISE * conc
    shear = SHEAR_LOW + SHEAR_RISE * conc
    dilation = EIGEN_STRAIN * conc
    d = [p - dilation for p in parts[:3]]
    trace = d[0] + d[1] + d[2]
    energy = d[0] * d[0] + d[1] * d[1] + d[2] * d[2]
    energy = energy + 2.0 * (parts[3] * parts[3] + parts[4] * parts[4] + parts[5] * parts[5])
    chemical = 2.0 * WELL_HEIGHT * conc * (1.0 - conc) * (1.0 - 2.0 * conc)
    return (
        chemical
        + 0.5 * FIRST_RISE * trace * trace
        + SHEAR_RISE * energy
        - EIGEN_STRAIN * (3.0 * first + 2.0 * shear) * trace
    )


def sum_squares(parts):
    total = parts[0] * parts[0]
    for part in parts[1:]:
        total = total + part * part
    return total


def fold(value):
    tile = value[0:8, 0:H] + value[0:8, H:N]
    for at in range(8, ROWS, 8):
        tile = tile + (value[at : at + 8, 0:H] + value[at : at + 8, H:N])
    return tile


ORDER = (YY, YZ, ZZ, XY, XZ, XX)
PRESSURE, CONC, FIRST, STRESS, SHIFT, DRIVE, NEXT = 0, 1, 2, 5, 10, 16, 17
FIELDS = 18
COLS, LINES = 16, 8
MESH = pl.DeviceIdType.MESH


def step_kernel(
    base_hbm,
    concentration_hbm,
    result,
    strain_out,
    norms,
    base,
    concentration,
    landed,
    sent,
    plain,
    cells,
    conc,
    work,
    before,
    kept,
    turned,
    spectrum,
    conc_hat,
    planes,
    lines,
    tall,
    wide,
    zf,
    zb,
    yf,
    yb,
    xf,
    xb,
    partial,
    col_sums,
    row_sums,
    send_sems,
    recv_sems,
    side_send,
    side_recv,
):
    row, col = lax.axis_index("row"), lax.axis_index("col")
    me = row * COLS + col
    next_col = lax.rem(col + 1, COLS)

    def tiles(ref, field, device):
        return ref.at[field, pl.ds(pl.multiple_of(device * 8, 8), 8), :]

    def row_at(step):
        return lax.rem(row + step, LINES)

    def each_device(step, act):
        for shift in range(1 if isinstance(step, int) and step == 0 else 0, COLS):
            act(row_at(step), lax.rem(col + shift, COLS))

    def send_row(field, step):
        def go(other_row, other_col):
            other = other_row * COLS + other_col
            pltpu.make_async_remote_copy(
                src_ref=tiles(sent, field, other),
                dst_ref=tiles(landed, field, me),
                send_sem=send_sems.at[field],
                recv_sem=recv_sems.at[field],
                device_id=(other_row, other_col),
                device_id_type=MESH,
            ).start()

        each_device(step, go)

    def keep_own(field):
        own = pl.ds(pl.multiple_of(me * 8, 8), 8)
        landed[field, own, :] = sent[field, own, :]

    def send_rows(field, low, high):
        def go(step, _):
            send_row(field, step)
            return 0

        lax.fori_loop(low, high, go, 0)

    def send(field):
        send_row(field, 0)

        def go(step, _):
            send_row(field, step)
            return 0

        lax.fori_loop(1, LINES, go, 0)
        keep_own(field)

    def scatter_send(field):
        scatter_block(sent, field, lines, row)
        send_row(field, 0)
        scatter_block(sent, field, lines, row_at(1))

        def go(step, _):
            send_row(field, step)
            scatter_block(sent, field, lines, row_at(step + 1))
            return 0

        lax.fori_loop(1, LINES - 1, go, 0)
        send_row(field, LINES - 1)
        keep_own(field)

    def whole(field):
        rows = pl.ds(0, 127 * 8)
        return pltpu.make_async_remote_copy(
            src_ref=sent.at[field, rows, :],
            dst_ref=landed.at[field, rows, :],
            send_sem=send_sems.at[field],
            recv_sem=recv_sems.at[field],
            device_id=(row, next_col),
            device_id_type=MESH,
        )

    def receive(field):
        whole(field).wait_recv()

    def side_copy(src, dst, index, device):
        return pltpu.make_async_remote_copy(
            src_ref=src,
            dst_ref=dst,
            send_sem=side_send.at[index],
            recv_sem=side_recv.at[index],
            device_id=device,
            device_id_type=MESH,
        )

    def column_send(src_of, dst, index):
        def go(i, _):
            target = lax.rem(col + i, COLS)
            side_copy(src_of(target), dst, index, (row, target)).start()
            return 0

        lax.fori_loop(1, COLS, go, 0)

    def lines_of(device):
        return pl.ds(pl.multiple_of(device * 16, 16), 16)

    def pair_of(device):
        return pl.ds(device * 2, 2)


    def cells_ahead(field, field_of):
        for half in range(2):
            value = z_ahead(field_of(half), zf, tall)
            for part in range(2):
                for j in range(2):
                    sent[field, pl.ds(part * 4 + 2 * half + j, H, stride=8), :] = value[
                        part * H : (part + 1) * H, j * H : (j + 1) * H
                    ]

    def cells_back(field, half):
        parts = [landed[field, pl.ds(i, H, stride=8), :] for i in range(8)]
        real = jnp.concatenate(parts[2 * half : 2 * half + 2], axis=1)
        imag = jnp.concatenate(parts[4 + 2 * half : 6 + 2 * half], axis=1)
        return z_back(real, imag, zb, tall)

    def plane_ahead(field, slot):
        gather_cells(landed, field, wide)
        lines[...] = dot(wide[...], yf[...])
        for part in range(2):
            put_tall(tall, part, lines[:, part * N : (part + 1) * N], slice(0, N))
        spectrum[slot] = dot(xf[...], tall[...])

    def plane_lines(value, factor=None):
        for part in range(2):
            rows = value[part * N : (part + 1) * N]
            if factor is not None:
                rows = factor * rows
            put_rows(wide, slice(0, N), part * N, rows)

    def plane_back():
        lines[...] = dot(wide[...], yb[...])

    concentration_in = pltpu.make_async_copy(concentration_hbm, concentration, side_send.at[10])
    concentration_in.start()
    base_in = pltpu.make_async_copy(base_hbm, base, side_send.at[11])
    base_in.start()
    barrier = pltpu.get_barrier_semaphore()

    def greet(other_row, other_col):
        pl.semaphore_signal(
            barrier, inc=1, device_id=(other_row, other_col), device_id_type=MESH
        )

    each_device(0, greet)

    def greet_row(step, _):
        each_device(step, greet)
        return 0

    lax.fori_loop(1, LINES, greet_row, 0)
    concentration_in.wait()
    base_in.wait()
    fill_z_ahead(base, zf)
    for half in range(2):
        block = concentration[16 * half : 16 * half + 16].reshape(N, N)
        cells[half] = block.T

    def first_pressure(half):
        return eigen_stress(cells[half])

    cells_ahead(PRESSURE, first_pressure)
    fill_right(base, yf, -1)
    fill_left(base, xf, 1)
    fill_left(base, xb, -1)
    pl.semaphore_wait(barrier, 127)
    send(PRESSURE)
    column_send(lambda t: concentration.at[pair_of(t)], plain.at[:, lines_of(col), :], 0)
    plain[:, lines_of(col), :] = concentration[pair_of(col)]
    plain_src, plain_dst = concentration.at[pl.ds(0, 30)], plain.at[:, pl.ds(0, 240), :]
    plain_wait = side_copy(plain_src, plain_dst, 0, (row, next_col))
    fill_z_back(base, zb)
    fill_right(base, yb, 1)
    cells_ahead(CONC, lambda half: cells[half])

    receive(PRESSURE)
    plane_ahead(PRESSURE, 3)
    green_first(spectrum, 3, me)

    def first_back(step, _):
        slot = 2 - step
        kept[slot] = x_lines(spectrum.at[slot], xb, tall)
        store_lines(sent, FIRST + slot, kept.at[slot])
        send(FIRST + slot)
        return 0

    lax.fori_loop(0, 3, first_back, 0)
    plain_wait.wait_recv()
    for x in range(2):
        conc[x] = plain[x].T

    wave_y, wave_z = lane_wave(H), row_wave_z()

    def first_strain(k, _):
        for slot, field, factor in (
            (0, 2, wave_y * wave_y),
            (1, 2, wave_y * wave_z),
            (2, 2, wave_z * wave_z),
            (3, 1, wave_y),
            (4, 1, wave_z),
            (5, 0, None),
        ):

            @pl.when(k == slot)
            def _():
                if slot in (0, 3, 5):
                    receive(FIRST + field)
                if slot == 5:
                    send_rows(CONC, 1, 5)
                for x in range(2):
                    real, imag = load_plane(landed, FIRST + field, x)
                    if factor is not None:
                        real, imag = factor * real, factor * imag
                    put_pair(wide, x, real, imag)

        plane_back()
        for x in range(2):
            rows = slice(x * H, (x + 1) * H)
            work[k, x] = z_back(lines[rows, 0:N], lines[rows, N : 2 * N], zb, tall)
        return 0

    lax.fori_loop(0, 6, first_strain, 0)
    partial[...] = jnp.zeros_like(partial)

    def stress(chunk, _):
        rows = pl.ds(chunk * ROWS, ROWS)
        for x in range(2):
            parts = [work[i, x, rows, :] for i in range(6)]
            partial[0] += sum_squares(parts)
            yy, yz, zz, xy, xz, xx = parts
            value = polarize([xx, yy, zz, yz, xz, xy], conc[x, rows, :])
            for i, which in enumerate(ORDER):
                work[i, x, rows, :] = value[which]
        return 0

    lax.fori_loop(0, N // ROWS, stress, 0)

    def stress_ahead(k, _):
        slot = jnp.where(k == 0, 5, jnp.where(k < 3, k + 2, k - 3))
        for x in range(2):
            value = z_ahead(work[slot, x], zf, tall)
            put_pair(wide, x, value[0:H], value[H:N])
        lines[...] = dot(wide[...], yf[...])

        @pl.when(k >= 3)
        def _():
            def mix(chunk, _):
                rows = pl.ds(chunk * ROWS, ROWS)
                index = chunk * ROWS + lax.broadcasted_iota(jnp.int32, (ROWS, N), 0)
                along_z = jnp.where(index < H, index, index - H).astype(F32) * STEP
                along_y = lane_wave(ROWS)
                for part in range(2):
                    lanes = slice(part * N, (part + 1) * N)
                    value = lines[rows, lanes]
                    lines[rows, lanes] = planes[rows, lanes] + along_z * value
                    planes[rows, lanes] = along_y * value
                return 0

            lax.fori_loop(0, N // ROWS, mix, 0)

        @pl.when(k != 3)
        def _():
            field = STRESS + jnp.where(k < 3, k, k - 1)
            store_planes(sent, field, lines)
            send(field)

        return 0

    planes[...] = jnp.zeros_like(planes)
    lax.fori_loop(0, 6, stress_ahead, 0)

    along_y, along_z = lane_wave(N), me.astype(F32) * STEP

    def first_planes(k, _):
        for which, field, factor in (
            (XX, 0, None),
            (YY, 2, along_y * along_y),
            (ZZ, 2, along_z * along_z),
            (YZ, 2, along_y * along_z),
            (XZ, 1, along_z),
            (XY, 1, along_y),
        ):

            @pl.when(k == which)
            def _():
                plane_lines(kept.at[field], factor)

        before[k] = dot(wide[...], yb[...])
        return 0

    lax.fori_loop(0, 6, first_planes, 0)

    def stress_x(slot, _):
        receive(STRESS + slot)
        x_ahead(landed, STRESS + slot, xf, tall, spectrum, slot)
        return 0

    lax.fori_loop(0, 5, stress_x, 0)
    send_row(CONC, 0)
    send_rows(CONC, 5, LINES)
    keep_own(CONC)
    green_full(spectrum, me)

    real_weight = jnp.where(me == 0, 1.0, 2.0) * float(N)
    imag_weight = jnp.where(me == 0, 0.0, 2.0) * float(N)

    def shift_back(slot, _):
        plane_lines(x_lines(spectrum.at[slot], xb, tall))
        plane_back()
        scatter_send(SHIFT + slot)

        def squares(chunk, _):
            rows = pl.ds(chunk * ROWS, ROWS)
            real = lines[rows, 0:N] - before[slot, rows, 0:N]
            imag = lines[rows, N : 2 * N] - before[slot, rows, N : 2 * N]
            partial[1] += real_weight * (real * real) + imag_weight * (imag * imag)
            return 0

        lax.fori_loop(0, N // ROWS, squares, 0)
        return 0

    lax.fori_loop(0, 6, shift_back, 0)

    col_sums[col, 0:8, :] = fold(partial[0])
    col_sums[col, 8:16, :] = fold(partial[1])
    column_send(lambda t: col_sums.at[col], col_sums.at[col], 1)
    sums_src = col_sums.at[pl.ds(0, COLS - 1)]
    col_wait = side_copy(sums_src, sums_src, 1, (row, next_col))

    def strain_copy(k):
        return pltpu.make_async_copy(turned.at[k], strain_out.at[k], side_send.at[3 + k])

    def second_strain(k, _):
        receive(SHIFT + k)
        for half in range(2):
            work[k, half] = cells_back(SHIFT + k, half)
        return 0

    lax.fori_loop(0, 6, second_strain, 0)

    def drive(chunk, _):
        rows = pl.ds(chunk * ROWS, ROWS)
        for half in range(2):
            parts = [work[i, half, rows, :] for i in range(6)]
            planes[rows, half * N : (half + 1) * N] = potential(parts, cells[half, rows, :])
        return 0

    lax.fori_loop(0, N // ROWS, drive, 0)
    cells_ahead(DRIVE, lambda half: planes[:, half * N : (half + 1) * N])
    send(DRIVE)

    def strain_turn(k, _):
        for half in range(2):
            turned[k, 16 * half : 16 * half + 16] = 2.0 * work[k, half].T.reshape(16, 16, N)
        strain_copy(k).start()
        return 0

    lax.fori_loop(0, 6, strain_turn, 0)
    receive(CONC)
    plane_ahead(CONC, 0)
    conc_hat[...] = spectrum[0]
    col_wait.wait_recv()
    total = col_sums[0]
    for i in range(1, COLS):
        total = total + col_sums[i]
    row_sums[row] = total

    def row_send(i, _):
        other = lax.rem(row + i, LINES)
        side_copy(row_sums.at[row], row_sums.at[row], 2, (other, col)).start()
        return 0

    lax.fori_loop(1, LINES, row_send, 0)
    rows_src = row_sums.at[pl.ds(0, LINES - 1)]
    row_wait = side_copy(rows_src, rows_src, 2, (lax.rem(row + 1, LINES), col))

    receive(DRIVE)
    plane_ahead(DRIVE, 0)
    relax(spectrum, 0, conc_hat, me)
    plane_lines(x_lines(spectrum.at[0], xb, tall))
    plane_back()
    scatter_send(NEXT)

    row_wait.wait_recv()
    total = row_sums[0]
    for i in range(1, LINES):
        total = total + row_sums[i]
    norms[...] = total
    row_wait.wait_send()
    col_wait.wait_send()
    plain_wait.wait_send()

    def sent_all(field, _):
        whole(field).wait_send()
        return 0

    lax.fori_loop(0, FIELDS, sent_all, 0)

    def strain_done(k, _):
        strain_copy(k).wait()
        return 0

    lax.fori_loop(0, 6, strain_done, 0)
    receive(NEXT)
    copies = []
    for half in range(2):
        planes_x = pl.ds(16 * half, 16)
        turned[0, planes_x] = 2.0 * cells_back(NEXT, half).T.reshape(16, 16, N)
        copies.append(
            pltpu.make_async_copy(
                turned.at[0, planes_x], result.at[planes_x], side_send.at[9 + half]
            )
        )
        copies[-1].start()
    for copy in copies:
        copy.wait()


def shape(*dims):
    return jax.ShapeDtypeStruct(dims, F32)


def shards(base, concentration):
    vmem = pl.BlockSpec(memory_space=pltpu.VMEM)
    hbm = pl.BlockSpec(memory_space=pl.ANY)
    hbm_in = pl.BlockSpec(memory_space=pltpu.HBM)
    result, strain, norms = pl.pallas_call(
        step_kernel,
        out_shape=[shape(32, 16, N), shape(6, 32, 16, N), shape(16, H)],
        in_specs=[hbm_in, hbm_in],
        out_specs=[hbm, hbm, vmem],
        scratch_shapes=[
            pltpu.VMEM((4, N, N), B16),
            pltpu.VMEM((32, 16, N), F32),
            pltpu.VMEM((FIELDS, 8 * H, H), F32),
            pltpu.VMEM((FIELDS, 8 * H, H), F32),
            pltpu.VMEM((2, N, N), F32),
            pltpu.VMEM((2, N, N), F32),
            pltpu.VMEM((2, N, N), F32),
            pltpu.VMEM((6, 2, N, N), F32),
            pltpu.VMEM((6, N, 2 * N), F32),
            pltpu.VMEM((3, 2 * N, N), F32),
            pltpu.VMEM((6, 32, 16, N), F32),
            pltpu.VMEM((6, 2 * N, N), F32),
            pltpu.VMEM((2 * N, N), F32),
            pltpu.VMEM((N, 2 * N), F32),
            pltpu.VMEM((N, 2 * N), F32),
            pltpu.VMEM((6 * N, N), B16),
            pltpu.VMEM((2 * H, 6 * N), B16),
            pltpu.VMEM((N, 3 * N), B16),
            pltpu.VMEM((N, 3 * N), B16),
            pltpu.VMEM((6 * N, 2 * N), B16),
            pltpu.VMEM((6 * N, 2 * N), B16),
            pltpu.VMEM((2 * N, 6 * N), B16),
            pltpu.VMEM((2 * N, 6 * N), B16),
            pltpu.VMEM((2, ROWS, N), F32),
            pltpu.VMEM((COLS, 16, H), F32),
            pltpu.VMEM((LINES, 16, H), F32),
            pltpu.SemaphoreType.DMA((FIELDS,)),
            pltpu.SemaphoreType.DMA((FIELDS,)),
            pltpu.SemaphoreType.DMA((12,)),
            pltpu.SemaphoreType.DMA((3,)),
        ],
        compiler_params=pltpu.CompilerParams(
            vmem_limit_bytes=48 * 2**20, has_side_effects=True, collective_id=0
        ),
        name="step",
    )(base, concentration)
    sums = jnp.sum(norms.reshape(2, 8 * H), axis=1)
    return 0.5 * result, 0.5 * strain, jnp.sqrt(sums * SCALE)


def solution(mesh):
    base = base_tables()
    body = jax.shard_map(
        shards,
        mesh=mesh,
        in_specs=(P(), P("row", "col", None)),
        out_specs=(P("row", "col", None), P(None, "row", "col", None), P()),
        check_vma=False,
    )

    def run(concentration):
        return body(jnp.asarray(base), concentration)

    return run
```
